512 devices in a mesh: patch: 512 (over y, x, z, core).
Axes of the slice: x: 4, y: 4, z: 16, core: 2. Of those that a mesh axis runs over, the one named last changes fastest.
Arguments:
- fields: float32 [4, 32, 32, 65536], P(None, None, None, 'patch'), may hold values from -1.5 to 4, as said below
- patch_level: int32 [65536], P('patch'), may hold values from 4 to 6
- relation: int32 [65536, 4], P('patch'), may hold values from 0 to 3
- face_half: int32 [65536, 4], P('patch'), may hold values from 0 to 1
- neighbour: int32 [65536, 4, 2], P('patch'), may hold values from 0 to 255, as said below
- send_list: int32 [512, 16, 8], P('patch'), may hold values from 0 to 127, as said below
Outputs:
- advanced: float32 [4, 32, 32, 65536], P(None, None, None, 'patch')
- time_step: float32 [], replicated
The draws below stay inside these ranges and needn't reach their ends.
Inputs may be any that keep to these rules, and one draw needn't show every extreme that they name: `send_list`: within each device's block for one curve distance the 8 entries are distinct local patches. `neighbour`: A reference of 128 or more names a slot of a device that exists on the curve. The second reference of a face is used only where relation is 3. `fields`: h lies in [2, 4], |hu| and |hv| at most 1.5, hc in [0, h].
All inputs are finite; a program needn't handle non-finite values.
Results may differ from the reference program's by a relative error of at most 0.0003.
Values sent between devices are 32-bit elements; how exact they have to be, the bound alone decides.
No kernel may reach another device: no remote copies, remote signals or barrier semaphores. Data moves between devices by JAX's collectives and lax.ppermute only.
A program may use at most 128 MiB of HBM per device.

```python
import jax
import jax.numpy as jnp
from jax import lax

CELLS = 32
HOPS = 8
P_DEV = 128
SEND = 8
NOFF = 16
POOL = 256
PATCHES = 65536
N_PATCH = 512


def draw_fields(key, part):
    keys = jax.random.split(key, 8)
    shape = (CELLS, CELLS, PATCHES)
    depth = jax.random.uniform(keys[1], shape, minval=2.0, maxval=4.0)
    flow_x = 0.5 * jax.random.truncated_normal(keys[3], -3.0, 3.0, shape)
    flow_y = 0.5 * jax.random.truncated_normal(keys[5], -3.0, 3.0, shape)
    tracer = depth * jax.random.uniform(keys[6], shape)
    return jnp.stack([depth, flow_x, flow_y, tracer]).astype(jnp.float32)


def draw_neighbour(key, part):
    keys = jax.random.split(key, 4)
    shape = (PATCHES, 4, 2)
    devices = PATCHES // P_DEV
    owner = (jnp.arange(PATCHES, dtype=jnp.int32) // P_DEV)[:, None, None]
    local = jax.random.randint(keys[0], shape, 0, P_DEV)
    block_index = jax.random.randint(keys[1], shape, 0, NOFF)
    slot = jax.random.randint(keys[2], shape, 0, SEND)
    remote = jax.random.randint(keys[3], shape, 0, 2) == 1
    distance = jnp.where(block_index < HOPS, block_index + 1, HOPS - 1 - block_index)
    source = owner - distance
    usable = remote & (source >= 0) & (source < devices)
    return jnp.where(usable, P_DEV + block_index * SEND + slot, local).astype(jnp.int32)


def draw_send_list(key, part):
    devices = PATCHES // P_DEV
    scores = jax.random.randint(key, (devices, NOFF, P_DEV), 0, 1 << 20) * P_DEV + jnp.arange(P_DEV, dtype=jnp.int32)
    order = jnp.argsort(scores, axis=-1, stable=True)
    return order[..., :SEND].astype(jnp.int32)


def touch_ends(values, rng, low, top_value):
    shape = values.shape
    spot = [jax.random.randint(jax.random.fold_in(rng, axis), (), 0, shape[axis]) for axis in range(len(shape))]
    values = values.at[tuple(spot)].set(low)
    longest = shape.index(max(shape))
    spot[longest] = (spot[longest] + 1) % shape[longest]
    return values.at[tuple(spot)].set(top_value)


def setup_inputs(seed: int = 0) -> dict:
    key_list = jax.random.split(jax.random.key(seed), 7)
    fields = draw_fields(jax.random.fold_in(key_list[6], 71), 0)
    patch_level = touch_ends(jax.random.randint(key_list[1], (PATCHES,), 4, 7), jax.random.fold_in(key_list[1], 1), 4, 6).astype(jnp.int32)
    relation = touch_ends(jax.random.randint(key_list[2], (PATCHES, 4), 0, 4), jax.random.fold_in(key_list[2], 1), 0, 3).astype(jnp.int32)
    face_half = touch_ends(jax.random.randint(key_list[3], (PATCHES, 4), 0, 2), jax.random.fold_in(key_list[3], 1), 0, 1).astype(jnp.int32)
    neighbour = draw_neighbour(jax.random.fold_in(key_list[6], 71), 0)
    send_list = draw_send_list(jax.random.fold_in(key_list[6], 71), 0)
    return dict(fields=fields, patch_level=patch_level, relation=relation, face_half=face_half, neighbour=neighbour, send_list=send_list)


courant = 0.4
finest_level = 6.0

def face_strips(state):
    west_side = state[:, 0:4]
    east_side = state[:, ::-1][:, 0:4]
    south_side = jnp.swapaxes(state[:, :, 0:4], 1, 2)
    north_side = jnp.swapaxes(state[:, :, ::-1][:, :, 0:4], 1, 2)
    stacked = jnp.stack([west_side, east_side, south_side, north_side])
    return jnp.transpose(stacked, (4, 0, 1, 2, 3))

def restrict(strip):
    total = strip[..., 0::2, 0::2] + strip[..., 1::2, 0::2]
    total = total + strip[..., 0::2, 1::2]
    total = total + strip[..., 1::2, 1::2]
    return 0.25 * total

def cell_speed(state):
    depth = state[0]
    return jnp.maximum(jnp.abs(state[1] / depth), jnp.abs(state[2] / depth)) + jnp.sqrt(depth)

def fill_ghosts(near, coarse, own_near, relation, face_half):
    cells = near.shape[-1]
    middle = cells // 2
    same_level = near[:, :, 0]
    column = near[:, :, 0, :, 0, :]
    padded = jnp.concatenate([column[..., :1], column, column[..., -1:]], axis=-1)
    slope = padded[..., 2:] - padded[..., :-2]
    upper_half = (face_half == 1)[:, :, None, None]
    base_value = jnp.where(upper_half, column[..., middle:], column[..., :middle])
    base_slope = jnp.where(upper_half, slope[..., middle:], slope[..., :middle])
    base_value = jnp.repeat(base_value, 2, axis=-1)
    base_slope = jnp.repeat(base_slope, 2, axis=-1)
    weights = jnp.where(jnp.arange(cells) % 2 == 1, 0.125, -0.125).astype(near.dtype)
    interpolated = base_value + weights * base_slope
    coarser = jnp.broadcast_to(interpolated[:, :, :, None, :], same_level.shape)
    finer_ghost = jnp.concatenate([coarse[:, :, 0], coarse[:, :, 1]], axis=-1)
    mirror_sign = jnp.array([[1.0, -1.0, 1.0, 1.0], [1.0, -1.0, 1.0, 1.0], [1.0, 1.0, -1.0, 1.0], [1.0, 1.0, -1.0, 1.0]], near.dtype)
    mirror = own_near * mirror_sign[None, :, :, None, None]
    choose = relation[:, :, None, None, None]
    return jnp.where(choose == 0, mirror, jnp.where(choose == 1, same_level, jnp.where(choose == 2, coarser, finer_ghost)))

def physical(state, normal):
    depth = state[0]
    velocity = state[normal] / depth
    components = [state[normal], state[1] * velocity, state[2] * velocity, state[3] * velocity]
    components[normal] = components[normal] + 0.5 * depth * depth
    return (jnp.stack(components), jnp.abs(velocity) + jnp.sqrt(depth))

def flux_change(padded, normal):
    centre = padded[:, 1:-1]
    slope = 0.5 * (padded[:, 2:] - padded[:, :-2])
    left_state = (centre + 0.5 * slope)[:, :-1]
    right_state = (centre - 0.5 * slope)[:, 1:]
    left_flux, left_speed = physical(left_state, normal)
    right_flux, right_speed = physical(right_state, normal)
    widest = jnp.maximum(left_speed, right_speed)
    numeric_flux = 0.5 * (left_flux + right_flux) - 0.5 * widest * (right_state - left_state)
    return numeric_flux[:, 1:] - numeric_flux[:, :-1]

def advance(state, ghosts, step_ratio):
    sides = jnp.transpose(ghosts, (1, 2, 3, 4, 0))
    along_x = jnp.concatenate([sides[0][:, ::-1], state, sides[1]], axis=1)
    along_y = jnp.concatenate([sides[2][:, ::-1], jnp.swapaxes(state, 1, 2), sides[3]], axis=1)
    change = flux_change(along_x, 1) + jnp.swapaxes(flux_change(along_y, 2), 1, 2)
    return state - step_ratio * change

def reference(fields, patch_level, relation, face_half, neighbour, send_list):
    nfields = fields.shape[0]
    cells = fields.shape[1]
    spacing = jnp.exp2(finest_level - patch_level.astype(jnp.float32))
    top_speed = lax.optimization_barrier(jnp.max(cell_speed(fields), axis=(0, 1)))
    time_step = courant * jnp.min(spacing / top_speed)
    step_ratio = time_step / spacing
    packs = face_strips(fields).reshape(PATCHES, -1)
    offsets = jnp.array(list(range(1, HOPS + 1)) + [-(value + 1) for value in range(HOPS)], jnp.int32)
    opposite = jnp.array([1, 0, 3, 2], jnp.int32)[None, :, None]

    def one_device(device):
        start = (device * P_DEV).astype(jnp.int32)
        state = lax.dynamic_slice_in_dim(fields, start, P_DEV, 3)
        own_pack = lax.dynamic_slice_in_dim(packs, start, P_DEV, 0)
        source = jnp.clip(device - offsets, 0, N_PATCH - 1).astype(jnp.int32)
        chosen = send_list[source, jnp.arange(NOFF, dtype=jnp.int32)]
        rows = (source[:, None] * P_DEV + chosen).reshape(-1).astype(jnp.int32)
        ghost_pool = jnp.concatenate([own_pack, packs[rows]], axis=0)
        refs = lax.dynamic_slice_in_dim(neighbour, start, P_DEV, 0)
        kinds = lax.dynamic_slice_in_dim(relation, start, P_DEV, 0)
        halves = lax.dynamic_slice_in_dim(face_half, start, P_DEV, 0)
        picked = ghost_pool.reshape(POOL, 4, -1)[refs, opposite]
        whole = picked.reshape(P_DEV, 4, 2, nfields, 4, cells)
        ghosts = fill_ghosts(whole[..., 0:2, :], restrict(whole), face_strips(state)[..., 0:2, :], kinds, halves)
        return advance(state, ghosts, lax.dynamic_slice_in_dim(step_ratio, start, P_DEV, 0))
    stacked = lax.map(one_device, jnp.arange(N_PATCH, dtype=jnp.int32))
    advanced = jnp.transpose(stacked, (1, 2, 3, 0, 4)).reshape(nfields, cells, cells, PATCHES)
    return (advanced, time_step)
```

```python
import jax
import jax.numpy as jnp
from jax import lax
from jax.experimental import pallas as pl
from jax.experimental.pallas import tpu as pltpu
from jax.sharding import Mesh
from jax.sharding import PartitionSpec as P

AXES = ("patch_0", "patch_1", "patch_2", "patch_3")
SHAPE = (4, 4, 16, 2)
COURANT = 0.4
CHUNKS = 8
NEAR = 64
ROWS = 80
PACK = 16 * ROWS
TILES = PACK // 128
LINE = 36
SPAN = 1160
F32 = jnp.float32
VMEM = pl.BlockSpec(memory_space=pltpu.VMEM)
ANY = pl.BlockSpec(memory_space=pl.ANY)


def spacing_of(level):
    return jnp.where(level == 6, 1.0, jnp.where(level == 5, 2.0, 4.0)).astype(F32)


def start_fields(fields, cells, sems, lead):
    width = 1024 // CHUNKS
    copies = []
    for chunk in range(CHUNKS):
        copy = pltpu.make_async_copy(
            fields.at[:, pl.ds(chunk * width, width)],
            cells.at[:, pl.ds(32 * lead + chunk * width, width)],
            sems.at[chunk],
        )
        copy.start()
        copies.append(copy)
    return copies


def core_index():
    return lax.axis_index("patch_3")


def pack_kernel(fields, level, send, own, swap, least, rows, cells, sems):
    copies = start_fields(fields, cells, sems, 0)
    width = 32 // CHUNKS
    fastest = jnp.zeros((32, 128), F32)
    for chunk in range(CHUNKS):
        copies[chunk].wait()

        def speeds(x, best):
            h, m, n = [cells[c, pl.ds(pl.multiple_of(32 * x, 32), 32), :] for c in range(3)]
            v = jnp.maximum(jnp.abs(m), jnp.abs(n)) / h
            return jnp.maximum(best, v + jnp.sqrt(h))

        fastest = lax.fori_loop(chunk * width, (chunk + 1) * width, speeds, fastest, unroll=True)
    top = jnp.max(fastest, axis=0, keepdims=True)
    ratio = spacing_of(level[...]) / top
    least[...] = jnp.broadcast_to(jnp.min(ratio, axis=1, keepdims=True), least.shape)

    for face in range(4):
        for c in range(4):
            base = (face * 4 + c) * ROWS
            at = [k if face % 2 == 0 else 31 - k for k in range(4)]
            for k in range(2):
                if face < 2:
                    line = cells[c, pl.ds(32 * at[k], 32), :]
                else:
                    line = cells[c, pl.ds(at[k], 32, stride=32), :]
                rows[pl.ds(base + 32 * k, 32), :] = line
            if face < 2:
                take = lambda k, odd: cells[c, pl.ds(at[k] * 32 + odd, 16, stride=2), :]
            else:
                take = lambda k, odd: cells[c, pl.ds(odd * 32 + at[k], 16, stride=64), :]
            total = take(2, 0) + take(3, 0)
            total = total + take(2, 1)
            total = total + take(3, 1)
            rows[pl.ds(base + NEAR, 16), :] = 0.25 * total

    lane = lax.broadcasted_iota(jnp.int32, (16, 128), 1)
    block = lax.broadcasted_iota(jnp.int32, (16, 128), 0)
    spread = jnp.where(((lane // 8) ^ (8 * core_index())) == block, 1.0, 0.0).astype(F32)
    listed = jnp.dot(send[...].astype(F32), spread, preferred_element_type=F32)
    slot = lax.broadcasted_iota(jnp.int32, (8, 128), 0)
    mine = (lax.broadcasted_iota(jnp.int32, (8, 128), 1) % 8) == slot
    chosen = jnp.sum(jnp.where(mine, listed, 0.0), axis=0, keepdims=True).astype(jnp.int32)
    index = jnp.broadcast_to(chosen, (128, 128))
    for tile in range(TILES):
        picked = jnp.take_along_axis(rows[pl.ds(tile * 128, 128), :], index, axis=1)
        turned = picked.T
        swap[80 + tile] = turned[0:8]
        for j in range(1, 8):
            own[(j - 1) * TILES + tile] = turned[8 * j : 8 * j + 8]
        for j in range(8):
            swap[j * TILES + tile] = turned[64 + 8 * j : 72 + 8 * j]


def pack(fields, level, send):
    return pl.pallas_call(
        pack_kernel,
        out_shape=(
            jax.ShapeDtypeStruct((70, 8, 128), F32),
            jax.ShapeDtypeStruct((90, 8, 128), F32),
            jax.ShapeDtypeStruct((lax.axis_size("patch_2"), 128), F32),
            jax.ShapeDtypeStruct((PACK, 128), F32),
        ),
        in_specs=[ANY, VMEM, VMEM],
        out_specs=(VMEM, VMEM, VMEM, VMEM),
        scratch_shapes=[pltpu.VMEM((4, 1024, 128), F32), pltpu.SemaphoreType.DMA((CHUNKS,))],
        name="pack",
    )(fields, level, send)


def least_kernel(got, out):
    low = jnp.min(jnp.min(got[...], axis=0, keepdims=True), axis=1, keepdims=True)
    out[...] = jnp.broadcast_to(low, out.shape)


def spread_least(got, members):
    return pl.pallas_call(
        least_kernel,
        out_shape=jax.ShapeDtypeStruct((members, 128), F32),
        in_specs=[VMEM],
        out_specs=VMEM,
        name="least",
    )(got)


def physical(q, normal):
    h = q[0]
    m = q[normal]
    v = m / h
    flux = [m, q[1] * v, q[2] * v, q[3] * v]
    flux[normal] = flux[normal] + 0.5 * h * h
    return flux, jnp.abs(v) + jnp.sqrt(h)


def interface(left, right, normal):
    lf, ls = physical(left, normal)
    rf, rs = physical(right, normal)
    widest = 0.5 * jnp.maximum(ls, rs)
    return [0.5 * (lf[c] + rf[c]) - widest * (right[c] - left[c]) for c in range(4)]


def step_kernel(
    fields, rows, r1, r2, r3, r4, w, q, got, level, relation, half, refs,
    out, step, cells, lines, fluxes, pool, edge, weave, sems,
):
    copies = start_fields(fields, cells, sems, 2)
    b8 = TILES
    sources = [
        (r1, b8), (r1, 0), (r2, b8), (r2, 0), (r3, b8), (r3, 0), (r4, b8), (r4, 0),
        (w, 80), (q, b8), (q, 0), (q, 3 * b8), (q, 2 * b8), (q, 5 * b8), (q, 4 * b8), (q, 6 * b8),
    ]
    for tile in range(TILES):
        joined = jnp.concatenate([ref[at + tile] for ref, at in sources], axis=0)
        pool[pl.ds(tile * 128, 128), :] = joined.T

    for copy in copies:
        copy.wait()

    def lay(x, carry):
        for c in range(4):
            line = cells[c, pl.ds(pl.multiple_of(32 * x + 64, 32), 32), :]
            lines[pl.ds(c * SPAN + x * LINE + 2, 32), :] = line
        return carry

    lax.fori_loop(0, 32, lay, 0, unroll=4)

    flip = 64 * core_index()
    for face in range(4):
        kind = relation[pl.ds(face, 1), :]
        upper = half[pl.ds(face, 1), :] == 1
        names = [refs[pl.ds(2 * face + m, 1), :] for m in range(2)]
        away = [name >= 128 for name in names]
        local = [name & 127 for name in names]
        remote = [(name & 127) ^ flip for name in names]

        def gather(own_rows, pool_rows, m):
            shape = own_rows.shape
            a = jnp.take_along_axis(own_rows, jnp.broadcast_to(local[m], shape), axis=1)
            b = jnp.take_along_axis(pool_rows, jnp.broadcast_to(remote[m], shape), axis=1)
            return jnp.where(away[m], b, a)

        for c in range(4):
            base = ((face ^ 1) * 4 + c) * ROWS

            def coarse_first(ref):
                total = ref[pl.ds(base, 16, stride=2), :] + ref[pl.ds(base + 32, 16, stride=2), :]
                total = total + ref[pl.ds(base + 1, 16, stride=2), :]
                total = total + ref[pl.ds(base + 33, 16, stride=2), :]
                return 0.25 * total

            near = gather(rows[pl.ds(base, NEAR), :], pool[pl.ds(base, NEAR), :], 0)
            fine = [[], []]
            pairs = [
                (coarse_first(rows), coarse_first(pool)),
                (rows[pl.ds(base + NEAR, 16), :], pool[pl.ds(base + NEAR, 16), :]),
            ]
            for g in range(2):
                fine[g] = jnp.concatenate([gather(*pairs[g], 0), gather(*pairs[g], 1)], axis=0)
            column = near[0:32]
            edge[pl.ds(1, 32), :] = column
            edge[pl.ds(0, 1), :] = column[0:1]
            edge[pl.ds(33, 1), :] = column[31:32]
            slope = edge[pl.ds(2, 32), :] - edge[pl.ds(0, 32), :]
            value = jnp.where(upper, column[16:32], column[0:16])
            tilt = 0.125 * jnp.where(upper, slope[16:32], slope[0:16])
            weave[pl.ds(0, 16, stride=2), :] = value - tilt
            weave[pl.ds(1, 16, stride=2), :] = value + tilt
            coarse = weave[...]
            sign = -1.0 if c == 1 + face // 2 else 1.0
            for g in range(2):
                mirror = sign * rows[pl.ds((face * 4 + c) * ROWS + 32 * g, 32), :]
                ghost = jnp.where(
                    kind == 0,
                    mirror,
                    jnp.where(
                        kind == 1,
                        near[32 * g : 32 * g + 32],
                        jnp.where(kind == 2, coarse, fine[g]),
                    ),
                )
                at = 1 - g if face % 2 == 0 else 34 + g
                if face < 2:
                    cells[c, pl.ds(32 * at, 32), :] = ghost
                else:
                    lines[pl.ds(c * SPAN + at, 32, stride=LINE), :] = ghost

    def along_y(n, carry):
        r = 1 + 8 * n
        left, right = [], []
        for c in range(4):
            before, here, after, beyond = [
                lines[pl.ds(c * SPAN + r + d, 8), :] for d in (-1, 0, 1, 2)
            ]
            left.append(here + 0.25 * (after - before))
            right.append(after - 0.25 * (beyond - here))
        flux = interface(left, right, 2)
        for c in range(4):
            fluxes[pl.ds(c * SPAN + r, 8), :] = flux[c]
        return carry

    lax.fori_loop(0, 144, along_y, 0, unroll=4)

    low = jnp.min(jnp.min(got[...], axis=0, keepdims=True), axis=1, keepdims=True)
    chosen = COURANT * low
    step[...] = chosen
    ratio = chosen / spacing_of(level[...])

    for part in range(4):
        y = 8 * part

        def load(x):
            return [cells[c, pl.ds(pl.multiple_of(32 * x + y, 8), 8), :] for c in range(4)]

        def along_x(i, carry):
            here, ahead, left, last = carry
            beyond = load(i + 3)
            lean = [0.25 * (beyond[c] - here[c]) for c in range(4)]
            right = [ahead[c] - lean[c] for c in range(4)]
            flux = interface(left, right, 1)
            if last is not None:
                for c in range(4):
                    at = c * SPAN + (i - 1) * LINE + y
                    change = (flux[c] - last[c]) + (
                        fluxes[pl.ds(at + 2, 8), :] - fluxes[pl.ds(at + 1, 8), :]
                    )
                    to = pl.multiple_of(32 * (i - 1) + y, 8)
                    out[c, pl.ds(to, 8), :] = here[c] - ratio * change
            return ahead, beyond, [ahead[c] + lean[c] for c in range(4)], flux

        first, second, third = load(0), load(1), load(2)
        left = [second[c] + 0.25 * (third[c] - first[c]) for c in range(4)]
        state = along_x(0, (second, third, left, None))
        lax.fori_loop(1, 33, along_x, state, unroll=4)


def advance(*operands):
    return pl.pallas_call(
        step_kernel,
        out_shape=(
            jax.ShapeDtypeStruct((4, 1024, 128), F32),
            jax.ShapeDtypeStruct((1, 1), F32),
        ),
        in_specs=[ANY] + [VMEM] * 12,
        out_specs=(VMEM, VMEM),
        scratch_shapes=[
            pltpu.VMEM((4, 36 * 32, 128), F32),
            pltpu.VMEM((4 * SPAN, 128), F32),
            pltpu.VMEM((4 * SPAN, 128), F32),
            pltpu.VMEM((PACK, 128), F32),
            pltpu.VMEM((40, 128), F32),
            pltpu.VMEM((32, 128), F32),
            pltpu.SemaphoreType.DMA((CHUNKS,)),
        ],
        name="advance",
    )(*operands)


def two_way(array, chips):
    n = lax.axis_size(AXES)
    pairs = [(i, (i + (2 * chips if i % 2 == 0 else -2 * chips)) % n) for i in range(n)]
    return lax.ppermute(array, AXES, pairs)


def swap_cores(array):
    return lax.ppermute(array, AXES, [(i, i ^ 1) for i in range(lax.axis_size(AXES))])


def on_device(fields, patch_level, relation, face_half, neighbour, send_list):
    level = patch_level.reshape(1, 128)
    flat = fields.reshape(4, 1024, 128)
    own, swap, least, rows = pack(flat, level, send_list[0].T)
    w = swap_cores(swap)

    def blk(array, n):
        return array[n * TILES : (n + 1) * TILES]

    moved = []
    for chips in range(1, 5):
        a = 2 * chips - 2
        parts = [blk(own, a), blk(w, a)]
        if chips < 4:
            parts.append(blk(own, a + 1))
        parts.append(blk(w, a + 1))
        moved.append(two_way(jnp.concatenate(parts), chips))
    q = swap_cores(jnp.concatenate([array[2 * TILES :] for array in moved]))
    got = lax.all_to_all(least, ("patch_2",), 0, 0, tiled=True)
    others = ("patch_0", "patch_1", "patch_3")
    got = lax.all_to_all(spread_least(got, lax.axis_size(others)), others, 0, 0, tiled=True)
    advanced, step = advance(
        flat, rows, *moved, w, q, got, level, relation.T, face_half.T,
        neighbour.transpose(1, 2, 0).reshape(8, 128),
    )
    return advanced.reshape(fields.shape), step[0, 0]


def solution(mesh):
    split = Mesh(mesh.devices.reshape(SHAPE), AXES)
    return jax.shard_map(
        on_device,
        mesh=split,
        in_specs=(
            P(None, None, None, AXES),
            P(AXES),
            P(AXES, None),
            P(AXES, None),
            P(AXES, None, None),
            P(AXES, None, None),
        ),
        out_specs=(P(None, None, None, AXES), P()),
        check_vma=False,
    )
```

```python
import jax
import jax.numpy as jnp
from jax import lax
from jax.experimental import pallas as pl
from jax.experimental.pallas import tpu as pltpu
from jax.sharding import Mesh
from jax.sharding import PartitionSpec as P

AXES = ("patch_0", "patch_1", "patch_2", "patch_3")
SHAPE = (4, 4, 16, 2)
COURANT = 0.4
CHUNKS = 8
NEAR = 64
ROWS = 80
PACK = 16 * ROWS
DEEP = 2 * 4 * 2 * 32
T = PACK // 128
LINE = 36
SPAN = 1160
F32 = jnp.float32
VMEM = pl.BlockSpec(memory_space=pltpu.VMEM)
ANY = pl.BlockSpec(memory_space=pl.ANY)


def spacing_of(level):
    return jnp.where(level == 6, 1.0, jnp.where(level == 5, 2.0, 4.0)).astype(F32)


def start_chunks(source, target, sems, inward=True):
    width = 1024 // CHUNKS
    copies = []
    for chunk in range(CHUNKS):
        part = pl.ds(chunk * width, width)
        copies.append(pltpu.make_async_copy(source.at[:, part], target.at[:, part], sems.at[chunk]))
        if inward:
            copies[-1].start()
    return copies


def core_index():
    return lax.axis_index("patch_3")


def pack_kernel(fields, level, send, own, swap, rows, deep, cells, sems):
    copies = start_chunks(fields, cells, sems)
    width = 32 // CHUNKS
    fastest = jnp.zeros((32, 128), F32)
    for chunk in range(CHUNKS):
        copies[chunk].wait()

        def speeds(x, best):
            h, m, n = [cells[c, pl.ds(pl.multiple_of(32 * x, 32), 32), :] for c in range(3)]
            v = jnp.maximum(jnp.abs(m), jnp.abs(n)) / h
            return jnp.maximum(best, v + jnp.sqrt(h))

        fastest = lax.fori_loop(chunk * width, (chunk + 1) * width, speeds, fastest, unroll=True)
    top = jnp.max(fastest, axis=0, keepdims=True)
    ratio = spacing_of(level[...]) / top
    swap[9 * T] = jnp.broadcast_to(jnp.min(ratio, axis=1, keepdims=True), (8, 128))

    for face in range(4):
        for c in range(4):
            base = (face * 4 + c) * ROWS
            at = [k if face % 2 == 0 else 31 - k for k in range(4)]
            inner = ((face - 2) * 4 + c) * 64
            for k in range(4):
                if face < 2 and k < 2:
                    rows[pl.ds(base + 32 * k, 32), :] = cells[c, pl.ds(32 * at[k], 32), :]
                if face >= 2:
                    line = cells[c, pl.ds(at[k], 32, stride=32), :]
                    if k < 2:
                        rows[pl.ds(base + 32 * k, 32), :] = line
                    else:
                        deep[pl.ds(inner + 32 * (k - 2), 32), :] = line

            def take(k, odd):
                if face < 2:
                    return cells[c, pl.ds(at[k] * 32 + odd, 16, stride=2), :]
                return deep[pl.ds(inner + 32 * (k - 2) + odd, 16, stride=2), :]

            total = take(2, 0) + take(3, 0)
            total = total + take(2, 1)
            total = total + take(3, 1)
            rows[pl.ds(base + NEAR, 16), :] = 0.25 * total

    lane = lax.broadcasted_iota(jnp.int32, (16, 128), 1)
    block = lax.broadcasted_iota(jnp.int32, (16, 128), 0)
    spread = jnp.where(((lane // 8) ^ (8 * core_index())) == block, 1.0, 0.0).astype(F32)
    listed = jnp.dot(send[...].astype(F32), spread, preferred_element_type=F32)
    slot = lax.broadcasted_iota(jnp.int32, (8, 128), 0)
    mine = (lax.broadcasted_iota(jnp.int32, (8, 128), 1) % 8) == slot
    chosen = jnp.sum(jnp.where(mine, listed, 0.0), axis=0, keepdims=True).astype(jnp.int32)
    index = jnp.broadcast_to(chosen, (128, 128))
    for tile in range(T):
        picked = jnp.take_along_axis(rows[pl.ds(tile * 128, 128), :], index, axis=1)
        turned = picked.T
        swap[8 * T + tile] = turned[0:8]
        for j in range(1, 8):
            own[(j - 1) * T + tile] = turned[8 * j : 8 * j + 8]
        for j in range(8):
            swap[j * T + tile] = turned[64 + 8 * j : 72 + 8 * j]


def tiles(n):
    return jax.ShapeDtypeStruct((n, 8, 128), F32)


def pack(fields, level, send):
    return pl.pallas_call(
        pack_kernel,
        out_shape=(
            tiles(7 * T),
            tiles(9 * T + 1),
            jax.ShapeDtypeStruct((PACK, 128), F32),
            jax.ShapeDtypeStruct((DEEP, 128), F32),
        ),
        in_specs=[ANY, VMEM, VMEM],
        out_specs=(VMEM,) * 4,
        scratch_shapes=[pltpu.VMEM((4, 1024, 128), F32), pltpu.SemaphoreType.DMA((CHUNKS,))],
        name="pack",
    )(fields, level, send)


def physical(q, normal):
    h = q[0]
    m = q[normal]
    v = m / h
    flux = [m, q[1] * v, q[2] * v, q[3] * v]
    flux[normal] = flux[normal] + 0.5 * h * h
    return flux, jnp.abs(v) + jnp.sqrt(h)


def interface(left, right, normal):
    lf, ls = physical(left, normal)
    rf, rs = physical(right, normal)
    widest = 0.5 * jnp.maximum(ls, rs)
    return [0.5 * (lf[c] + rf[c]) - widest * (right[c] - left[c]) for c in range(4)]


def inner_kernel(fields, out, cells, lines, fluxes, sems):
    copies = start_chunks(fields, cells, sems)
    width = 32 // CHUNKS

    def lay(x, carry):
        for c in range(4):
            line = cells[c, pl.ds(pl.multiple_of(32 * x, 32), 32), :]
            lines[pl.ds(c * SPAN + x * LINE + 2, 32), :] = line
        return carry

    for chunk in range(CHUNKS):
        copies[chunk].wait()
        lax.fori_loop(chunk * width, (chunk + 1) * width, lay, 0, unroll=True)

    def along_y(n, carry):
        r = 1 + 8 * n
        left, right = [], []
        for c in range(4):
            before, here, after, beyond = [
                lines[pl.ds(c * SPAN + r + d, 8), :] for d in (-1, 0, 1, 2)
            ]
            left.append(here + 0.25 * (after - before))
            right.append(after - 0.25 * (beyond - here))
        flux = interface(left, right, 2)
        for c in range(4):
            fluxes[pl.ds(c * SPAN + r, 8), :] = flux[c]
        return carry

    lax.fori_loop(0, 144, along_y, 0, unroll=4)

    sub = lax.broadcasted_iota(jnp.int32, (8, 128), 0)
    for part in range(4):
        y = 8 * part

        def load(x):
            return [cells[c, pl.ds(pl.multiple_of(32 * x + y, 8), 8), :] for c in range(4)]

        def across(c, x):
            at = c * SPAN + x * LINE + y
            change = fluxes[pl.ds(at + 2, 8), :] - fluxes[pl.ds(at + 1, 8), :]
            if part == 0:
                change = jnp.where(sub >= 2, change, 0.0)
            if part == 3:
                change = jnp.where(sub < 6, change, 0.0)
            return change

        def store(c, x, value):
            out[c, pl.ds(pl.multiple_of(32 * x + y, 8), 8), :] = value

        def along_x(x, carry):
            here, ahead, left, last = carry
            beyond = load(x + 2)
            lean = [0.25 * (beyond[c] - here[c]) for c in range(4)]
            right = [ahead[c] - lean[c] for c in range(4)]
            flux = interface(left, right, 1)
            if last is not None:
                for c in range(4):
                    store(c, x, (flux[c] - last[c]) + across(c, x))
            return ahead, beyond, [ahead[c] + lean[c] for c in range(4)], flux

        first, second, third = load(0), load(1), load(2)
        left = [second[c] + 0.25 * (third[c] - first[c]) for c in range(4)]
        state = along_x(1, (second, third, left, None))
        lax.fori_loop(2, 30, along_x, state, unroll=4)
        for x in (0, 1, 30, 31):
            for c in range(4):
                store(c, x, across(c, x))


def inner(fields):
    return pl.pallas_call(
        inner_kernel,
        out_shape=jax.ShapeDtypeStruct((4, 1024, 128), F32),
        in_specs=[ANY],
        out_specs=VMEM,
        scratch_shapes=[
            pltpu.VMEM((4, 1024, 128), F32),
            pltpu.VMEM((4 * SPAN, 128), F32),
            pltpu.VMEM((4 * SPAN, 128), F32),
            pltpu.SemaphoreType.DMA((CHUNKS,)),
        ],
        name="inner",
    )(fields)


def step_kernel(
    fields, inside, rows, deep, r1, r2, r3, r4, w, q, got, level, relation, half, refs,
    out, step, cells, change, fresh, ghosts, pool, edge, weave, in_sems, change_sems, out_sems,
):
    field_copies = start_chunks(fields, cells, in_sems)
    change_copies = start_chunks(inside, change, change_sems)
    sources = [
        (r1, T), (r1, 0), (r2, T), (r2, 0), (r3, T), (r3, 0), (r4, T), (r4, 0),
        (w, 8 * T), (q, T), (q, 0), (q, 3 * T), (q, 2 * T), (q, 5 * T), (q, 4 * T), (q, 6 * T),
    ]
    for tile in range(T):
        joined = jnp.concatenate([ref[at + tile] for ref, at in sources], axis=0)
        pool[pl.ds(tile * 128, 128), :] = joined.T

    flip = 64 * core_index()
    for face in range(4):
        kind = relation[pl.ds(face, 1), :]
        upper = half[pl.ds(face, 1), :] == 1
        names = [refs[pl.ds(2 * face + m, 1), :] for m in range(2)]
        away = [name >= 128 for name in names]
        local = [name & 127 for name in names]
        remote = [(name & 127) ^ flip for name in names]

        def gather(own_rows, pool_rows, m):
            shape = own_rows.shape
            a = jnp.take_along_axis(own_rows, jnp.broadcast_to(local[m], shape), axis=1)
            b = jnp.take_along_axis(pool_rows, jnp.broadcast_to(remote[m], shape), axis=1)
            return jnp.where(away[m], b, a)

        for c in range(4):
            base = ((face ^ 1) * 4 + c) * ROWS

            def coarse_first(ref):
                total = ref[pl.ds(base, 16, stride=2), :] + ref[pl.ds(base + 32, 16, stride=2), :]
                total = total + ref[pl.ds(base + 1, 16, stride=2), :]
                total = total + ref[pl.ds(base + 33, 16, stride=2), :]
                return 0.25 * total

            near = gather(rows[pl.ds(base, NEAR), :], pool[pl.ds(base, NEAR), :], 0)
            pairs = [
                (coarse_first(rows), coarse_first(pool)),
                (rows[pl.ds(base + NEAR, 16), :], pool[pl.ds(base + NEAR, 16), :]),
            ]
            column = near[0:32]
            spot = 40 * (4 * face + c)
            edge[pl.ds(spot + 1, 32), :] = column
            edge[pl.ds(spot, 1), :] = column[0:1]
            edge[pl.ds(spot + 33, 1), :] = column[31:32]
            slope = edge[pl.ds(spot + 2, 32), :] - edge[pl.ds(spot, 32), :]
            value = jnp.where(upper, column[16:32], column[0:16])
            tilt = 0.125 * jnp.where(upper, slope[16:32], slope[0:16])
            turn = 32 * (4 * face + c)
            weave[pl.ds(turn, 16, stride=2), :] = value - tilt
            weave[pl.ds(turn + 1, 16, stride=2), :] = value + tilt
            coarse = weave[pl.ds(turn, 32), :]
            sign = -1.0 if c == 1 + face // 2 else 1.0
            for g in range(2):
                fine = jnp.concatenate([gather(*pairs[g], 0), gather(*pairs[g], 1)], axis=0)
                mirror = sign * rows[pl.ds((face * 4 + c) * ROWS + 32 * g, 32), :]
                ghosts[pl.ds(((face * 4 + c) * 2 + g) * 32, 32), :] = jnp.where(
                    kind == 0,
                    mirror,
                    jnp.where(
                        kind == 1,
                        near[32 * g : 32 * g + 32],
                        jnp.where(kind == 2, coarse, fine),
                    ),
                )

    for copy in field_copies + change_copies:
        copy.wait()

    for face in range(4):

        def border(j, carry):
            def part(c, depth):
                along = pl.multiple_of(8 * j, 8)
                if depth < 0:
                    return ghosts[pl.ds(((face * 4 + c) * 2 - depth - 1) * 32 + along, 8), :]
                if face < 2:
                    x = depth if face == 0 else 31 - depth
                    return cells[c, pl.ds(32 * x + along, 8), :]
                if depth < 2:
                    return rows[pl.ds((face * 4 + c) * ROWS + 32 * depth + along, 8), :]
                return deep[pl.ds(((face - 2) * 4 + c) * 64 + 32 * (depth - 2) + along, 8), :]

            depths = [-2, -1, 0, 1, 2, 3]
            if face % 2 == 1:
                depths = depths[::-1]
            q6 = [[part(c, depth) for c in range(4)] for depth in depths]
            lean = [[0.25 * (q6[i + 1][c] - q6[i - 1][c]) for c in range(4)] for i in range(1, 5)]
            flux = []
            for i in range(1, 4):
                left = [q6[i][c] + lean[i - 1][c] for c in range(4)]
                right = [q6[i + 1][c] - lean[i][c] for c in range(4)]
                flux.append(interface(left, right, 1 + face // 2))
            for i in range(2):
                depth = depths[i + 2]
                where = depth if face % 2 == 0 else 31 - depth
                for c in range(4):
                    extra = flux[i + 1][c] - flux[i][c]
                    if face < 2:
                        spot = pl.ds(pl.multiple_of(32 * where + 8 * j, 8), 8)
                    else:
                        spot = pl.ds(256 * j + where, 8, stride=32)
                    change[c, spot, :] = change[c, spot, :] + extra
            return carry

        lax.fori_loop(0, 4, border, 0, unroll=2)

    low = jnp.min(jnp.min(got[...], axis=0, keepdims=True), axis=1, keepdims=True)
    chosen = COURANT * low
    step[...] = chosen
    ratio = chosen / spacing_of(level[...])

    out_copies = start_chunks(fresh, out, out_sems, inward=False)
    width = 1024 // CHUNKS
    for chunk in range(CHUNKS):

        def update(n, carry):
            spot = pl.ds(pl.multiple_of(chunk * width + 32 * n, 32), 32)
            for c in range(4):
                fresh[c, spot, :] = cells[c, spot, :] - ratio * change[c, spot, :]
            return carry

        lax.fori_loop(0, width // 32, update, 0, unroll=True)
        out_copies[chunk].start()
    for copy in out_copies:
        copy.wait()


def advance(*operands):
    return pl.pallas_call(
        step_kernel,
        out_shape=(
            jax.ShapeDtypeStruct((4, 1024, 128), F32),
            jax.ShapeDtypeStruct((1, 1), F32),
        ),
        in_specs=[ANY] * 2 + [VMEM] * 13,
        out_specs=(ANY, VMEM),
        scratch_shapes=[
            pltpu.VMEM((4, 1024, 128), F32),
            pltpu.VMEM((4, 1024, 128), F32),
            pltpu.VMEM((4, 1024, 128), F32),
            pltpu.VMEM((16 * 2 * 32, 128), F32),
            pltpu.VMEM((PACK, 128), F32),
            pltpu.VMEM((16 * 40, 128), F32),
            pltpu.VMEM((16 * 32, 128), F32),
            pltpu.SemaphoreType.DMA((CHUNKS,)),
            pltpu.SemaphoreType.DMA((CHUNKS,)),
            pltpu.SemaphoreType.DMA((CHUNKS,)),
        ],
        name="advance",
    )(*operands)


def two_way(array, chips):
    n = lax.axis_size(AXES)
    pairs = [(i, (i + (2 * chips if i % 2 == 0 else -2 * chips)) % n) for i in range(n)]
    return lax.ppermute(array, AXES, pairs)


def swap_cores(array):
    return lax.ppermute(array, AXES, [(i, i ^ 1) for i in range(lax.axis_size(AXES))])


def cross(array):
    n = lax.axis_size(AXES)
    return lax.ppermute(array, AXES, [(i, (i + (-3 if i % 2 else 3)) % n) for i in range(n)])


def compute(fields, patch_level, relation, face_half, neighbour, send_list):
    level = patch_level.reshape(1, 128)
    flat = fields.reshape(4, 1024, 128)
    own, swap, rows, deep = pack(flat, level, send_list[0].T)
    w = swap_cores(swap)

    def blk(array, n, count=1):
        return array[n * T : (n + count) * T]

    def ahead(j):
        return blk(own, j - 2)

    def beside(j):
        return blk(w, j - 1)

    low = jnp.minimum(swap[9 * T :], w[9 * T :])
    r4 = two_way(jnp.concatenate([ahead(8), beside(7), low]), 4)
    inside = inner(flat)
    low = jnp.minimum(low, r4[2 * T :])
    r3 = two_way(jnp.concatenate([ahead(6), beside(5), beside(8), low]), 3)
    r2 = two_way(jnp.concatenate([ahead(4), beside(3), ahead(7), beside(6), low]), 2)
    r1 = two_way(jnp.concatenate([ahead(2), beside(1), ahead(5), beside(4), low]), 1)
    q = cross(
        jnp.concatenate([ahead(3), beside(2), blk(r1, 2, 2), blk(r2, 2, 2), blk(r3, 2)])
    )
    depth = lax.axis_size("patch_2")
    columns = lax.axis_size(("patch_0", "patch_1"))
    low = jnp.minimum(jnp.minimum(low, r1[4 * T :]), jnp.minimum(r2[4 * T :], r3[3 * T :]))
    least = jnp.broadcast_to(low[0, :1], (2 * columns, 128))
    groups = [
        [(r * depth + (g + c) % depth) * 2 + c for r in range(columns) for c in range(2)]
        for g in range(depth)
    ]
    got = lax.all_to_all(least, AXES, 0, 0, tiled=True, axis_index_groups=groups)
    advanced, step = advance(
        flat, inside, rows, deep, r1, r2, r3, r4, w, q, got, level, relation.T, face_half.T,
        neighbour.transpose(1, 2, 0).reshape(8, 128),
    )
    return advanced.reshape(fields.shape), step[0, 0]


def stepper(mesh):
    split = Mesh(mesh.devices.reshape(SHAPE), AXES)
    return jax.shard_map(
        compute,
        mesh=split,
        in_specs=(
            P(None, None, None, AXES),
            P(AXES),
            P(AXES, None),
            P(AXES, None),
            P(AXES, None, None),
            P(AXES, None, None),
        ),
        out_specs=(P(None, None, None, AXES), P()),
        check_vma=False,
    )


def solution(mesh):
    return stepper(mesh)
```

```python
import jax
import jax.numpy as jnp
from jax import lax
from jax.experimental import pallas as pl
from jax.experimental.pallas import tpu as pltpu
from jax.sharding import Mesh
from jax.sharding import PartitionSpec as P

AXES = ("patch_0", "patch_1", "patch_2", "patch_3")
SHAPE = (4, 4, 16, 2)
COURANT = 0.4
CHUNKS = 8
NEAR = 64
ROWS = 80
PACK = 16 * ROWS
DEEP = 2 * 4 * 2 * 32
T = PACK // 128
LINE = 36
SPAN = 1160
F32 = jnp.float32
VMEM = pl.BlockSpec(memory_space=pltpu.VMEM)
ANY = pl.BlockSpec(memory_space=pl.ANY)


def spacing_of(level):
    return jnp.where(level == 6, 1.0, jnp.where(level == 5, 2.0, 4.0)).astype(F32)


def start_chunks(source, target, sems):
    width = 1024 // CHUNKS
    copies = []
    for chunk in range(CHUNKS):
        part = pl.ds(chunk * width, width)
        copies.append(pltpu.make_async_copy(source.at[:, part], target.at[:, part], sems.at[chunk]))
        copies[-1].start()
    return copies


def core_index():
    return lax.axis_index("patch_3")


def pack_kernel(fields, level_in, send_in, own, swap, rows, deep, cells, level, send, sems, small):
    extras = [
        pltpu.make_async_copy(level_in, level, small.at[0]),
        pltpu.make_async_copy(send_in, send, small.at[1]),
    ]
    copies = start_chunks(fields, cells, sems)
    for extra in extras:
        extra.start()
    width = 32 // CHUNKS
    fastest = jnp.zeros((32, 128), F32)
    for chunk in range(CHUNKS):
        copies[chunk].wait()

        def speeds(x, best):
            h, m, n = [cells[c, pl.ds(pl.multiple_of(32 * x, 32), 32), :] for c in range(3)]
            v = jnp.maximum(jnp.abs(m), jnp.abs(n)) / h
            return jnp.maximum(best, v + jnp.sqrt(h))

        fastest = lax.fori_loop(chunk * width, (chunk + 1) * width, speeds, fastest, unroll=True)
    for extra in extras:
        extra.wait()
    top = jnp.max(fastest, axis=0, keepdims=True)
    ratio = spacing_of(level[...]) / top
    swap[9 * T] = jnp.broadcast_to(jnp.min(ratio, axis=1, keepdims=True), (8, 128))

    for face in range(4):
        for c in range(4):
            base = (face * 4 + c) * ROWS
            at = [k if face % 2 == 0 else 31 - k for k in range(4)]
            inner = ((face - 2) * 4 + c) * 64
            for k in range(4):
                if face < 2 and k < 2:
                    rows[pl.ds(base + 32 * k, 32), :] = cells[c, pl.ds(32 * at[k], 32), :]
                if face >= 2:
                    line = cells[c, pl.ds(at[k], 32, stride=32), :]
                    if k < 2:
                        rows[pl.ds(base + 32 * k, 32), :] = line
                    else:
                        deep[pl.ds(inner + 32 * (k - 2), 32), :] = line

            def take(k, odd):
                if face < 2:
                    return cells[c, pl.ds(at[k] * 32 + odd, 16, stride=2), :]
                return deep[pl.ds(inner + 32 * (k - 2) + odd, 16, stride=2), :]

            total = take(2, 0) + take(3, 0)
            total = total + take(2, 1)
            total = total + take(3, 1)
            rows[pl.ds(base + NEAR, 16), :] = 0.25 * total

    lane = lax.broadcasted_iota(jnp.int32, (16, 128), 1)
    block = lax.broadcasted_iota(jnp.int32, (16, 128), 0)
    spread = jnp.where(((lane // 8) ^ (8 * core_index())) == block, 1.0, 0.0).astype(F32)
    listed = jnp.dot(send[...].astype(F32), spread, preferred_element_type=F32)
    slot = lax.broadcasted_iota(jnp.int32, (8, 128), 0)
    mine = (lax.broadcasted_iota(jnp.int32, (8, 128), 1) % 8) == slot
    chosen = jnp.sum(jnp.where(mine, listed, 0.0), axis=0, keepdims=True).astype(jnp.int32)
    index = jnp.broadcast_to(chosen, (128, 128))
    for tile in range(T):
        picked = jnp.take_along_axis(rows[pl.ds(tile * 128, 128), :], index, axis=1)
        turned = picked.T
        swap[8 * T + tile] = turned[0:8]
        for j in range(1, 8):
            own[(j - 1) * T + tile] = turned[8 * j : 8 * j + 8]
        for j in range(8):
            swap[j * T + tile] = turned[64 + 8 * j : 72 + 8 * j]


def tiles(n):
    return jax.ShapeDtypeStruct((n, 8, 128), F32)


def pack(fields, level, send):
    return pl.pallas_call(
        pack_kernel,
        out_shape=(
            tiles(7 * T),
            tiles(9 * T + 1),
            jax.ShapeDtypeStruct((PACK, 128), F32),
            jax.ShapeDtypeStruct((DEEP, 128), F32),
        ),
        in_specs=[pl.BlockSpec(memory_space=pltpu.HBM)] * 3,
        out_specs=(VMEM,) * 4,
        scratch_shapes=[
            pltpu.VMEM((4, 1024, 128), F32),
            pltpu.VMEM((1, 128), jnp.int32),
            pltpu.VMEM((8, 16), jnp.int32),
            pltpu.SemaphoreType.DMA((CHUNKS,)),
            pltpu.SemaphoreType.DMA((2,)),
        ],
        compiler_params=pltpu.CompilerParams(vmem_limit_bytes=8 << 20),
        name="pack",
    )(*[pltpu.with_memory_space_constraint(a, pltpu.HBM) for a in (fields, level, send)])


def physical(q, normal):
    h = q[0]
    m = q[normal]
    v = m / h
    flux = [m, q[1] * v, q[2] * v, q[3] * v]
    flux[normal] = flux[normal] + 0.5 * h * h
    return flux, jnp.abs(v) + jnp.sqrt(h)


def interface(left, right, normal):
    lf, ls = physical(left, normal)
    rf, rs = physical(right, normal)
    widest = 0.5 * jnp.maximum(ls, rs)
    return [0.5 * (lf[c] + rf[c]) - widest * (right[c] - left[c]) for c in range(4)]


def inner_kernel(cells, out, lines, fluxes):
    def lay(x, carry):
        for c in range(4):
            line = cells[c, pl.ds(pl.multiple_of(32 * x, 32), 32), :]
            lines[pl.ds(c * SPAN + x * LINE + 2, 32), :] = line
        return carry

    lax.fori_loop(0, 32, lay, 0, unroll=4)

    def along_y(n, carry):
        r = 1 + 8 * n
        left, right = [], []
        for c in range(4):
            before, here, after, beyond = [
                lines[pl.ds(c * SPAN + r + d, 8), :] for d in (-1, 0, 1, 2)
            ]
            left.append(here + 0.25 * (after - before))
            right.append(after - 0.25 * (beyond - here))
        flux = interface(left, right, 2)
        for c in range(4):
            fluxes[pl.ds(c * SPAN + r, 8), :] = flux[c]
        return carry

    lax.fori_loop(0, 144, along_y, 0, unroll=4)

    sub = lax.broadcasted_iota(jnp.int32, (8, 128), 0)
    for part in range(4):
        y = 8 * part

        def load(x):
            return [cells[c, pl.ds(pl.multiple_of(32 * x + y, 8), 8), :] for c in range(4)]

        def across(c, x):
            at = c * SPAN + x * LINE + y
            change = fluxes[pl.ds(at + 2, 8), :] - fluxes[pl.ds(at + 1, 8), :]
            if part == 0:
                change = jnp.where(sub >= 2, change, 0.0)
            if part == 3:
                change = jnp.where(sub < 6, change, 0.0)
            return change

        def store(c, x, value):
            out[c, pl.ds(pl.multiple_of(32 * x + y, 8), 8), :] = value

        def along_x(x, carry):
            here, ahead, left, last = carry
            beyond = load(x + 2)
            lean = [0.25 * (beyond[c] - here[c]) for c in range(4)]
            right = [ahead[c] - lean[c] for c in range(4)]
            flux = interface(left, right, 1)
            if last is not None:
                for c in range(4):
                    store(c, x, (flux[c] - last[c]) + across(c, x))
            return ahead, beyond, [ahead[c] + lean[c] for c in range(4)], flux

        first, second, third = load(0), load(1), load(2)
        left = [second[c] + 0.25 * (third[c] - first[c]) for c in range(4)]
        state = along_x(1, (second, third, left, None))
        lax.fori_loop(2, 30, along_x, state, unroll=4)
        for x in (0, 1, 30, 31):
            for c in range(4):
                store(c, x, across(c, x))


def inner(fields):
    return pl.pallas_call(
        inner_kernel,
        out_shape=jax.ShapeDtypeStruct((4, 1024, 128), F32),
        in_specs=[VMEM],
        out_specs=VMEM,
        scratch_shapes=[pltpu.VMEM((4 * SPAN, 128), F32), pltpu.VMEM((4 * SPAN, 128), F32)],
        compiler_params=pltpu.CompilerParams(vmem_limit_bytes=14 << 20),
        name="inner",
    )(fields)


def step_kernel(
    cells, inside, rows, deep, r1, r2, r3, r4, w, q, got, level, relation, half, refs,
    out, step, fresh, ghosts, pool, edge, weave, out_sems,
):
    sources = [
        (r1, T), (r1, 0), (r2, T), (r2, 0), (r3, T), (r3, 0), (r4, T), (r4, 0),
        (w, 8 * T), (q, T), (q, 0), (q, 3 * T), (q, 2 * T), (q, 5 * T), (q, 4 * T), (q, 6 * T),
    ]
    for tile in range(T):
        joined = jnp.concatenate([ref[at + tile] for ref, at in sources], axis=0)
        pool[pl.ds(tile * 128, 128), :] = joined.T

    flip = 64 * core_index()
    for face in range(4):
        kind = relation[pl.ds(face, 1), :]
        upper = half[pl.ds(face, 1), :] == 1
        names = [refs[pl.ds(2 * face + m, 1), :] for m in range(2)]
        away = [name >= 128 for name in names]
        local = [name & 127 for name in names]
        remote = [(name & 127) ^ flip for name in names]

        def gather(own_rows, pool_rows, m):
            shape = own_rows.shape
            a = jnp.take_along_axis(own_rows, jnp.broadcast_to(local[m], shape), axis=1)
            b = jnp.take_along_axis(pool_rows, jnp.broadcast_to(remote[m], shape), axis=1)
            return jnp.where(away[m], b, a)

        for c in range(4):
            base = ((face ^ 1) * 4 + c) * ROWS

            def coarse_first(ref):
                total = ref[pl.ds(base, 16, stride=2), :] + ref[pl.ds(base + 32, 16, stride=2), :]
                total = total + ref[pl.ds(base + 1, 16, stride=2), :]
                total = total + ref[pl.ds(base + 33, 16, stride=2), :]
                return 0.25 * total

            near = gather(rows[pl.ds(base, NEAR), :], pool[pl.ds(base, NEAR), :], 0)
            pairs = [
                (coarse_first(rows), coarse_first(pool)),
                (rows[pl.ds(base + NEAR, 16), :], pool[pl.ds(base + NEAR, 16), :]),
            ]
            column = near[0:32]
            spot = 40 * (4 * face + c)
            edge[pl.ds(spot + 1, 32), :] = column
            edge[pl.ds(spot, 1), :] = column[0:1]
            edge[pl.ds(spot + 33, 1), :] = column[31:32]
            slope = edge[pl.ds(spot + 2, 32), :] - edge[pl.ds(spot, 32), :]
            value = jnp.where(upper, column[16:32], column[0:16])
            tilt = 0.125 * jnp.where(upper, slope[16:32], slope[0:16])
            turn = 32 * (4 * face + c)
            weave[pl.ds(turn, 16, stride=2), :] = value - tilt
            weave[pl.ds(turn + 1, 16, stride=2), :] = value + tilt
            coarse = weave[pl.ds(turn, 32), :]
            sign = -1.0 if c == 1 + face // 2 else 1.0
            for g in range(2):
                fine = jnp.concatenate([gather(*pairs[g], 0), gather(*pairs[g], 1)], axis=0)
                mirror = sign * rows[pl.ds((face * 4 + c) * ROWS + 32 * g, 32), :]
                ghosts[pl.ds(((face * 4 + c) * 2 + g) * 32, 32), :] = jnp.where(
                    kind == 0,
                    mirror,
                    jnp.where(
                        kind == 1,
                        near[32 * g : 32 * g + 32],
                        jnp.where(kind == 2, coarse, fine),
                    ),
                )

    low = jnp.min(jnp.min(got[...], axis=0, keepdims=True), axis=1, keepdims=True)
    chosen = COURANT * low
    step[...] = chosen
    ratio = chosen / spacing_of(level[...])

    def border(face, j):
        def part(c, depth):
            if depth < 0:
                return ghosts[pl.ds(((face * 4 + c) * 2 - depth - 1) * 32 + 8 * j, 8), :]
            if face < 2:
                x = depth if face == 0 else 31 - depth
                return cells[c, pl.ds(32 * x + 8 * j, 8), :]
            if depth < 2:
                return rows[pl.ds((face * 4 + c) * ROWS + 32 * depth + 8 * j, 8), :]
            return deep[pl.ds(((face - 2) * 4 + c) * 64 + 32 * (depth - 2) + 8 * j, 8), :]

        depths = [-2, -1, 0, 1, 2, 3]
        if face % 2 == 1:
            depths = depths[::-1]
        q6 = [[part(c, depth) for c in range(4)] for depth in depths]
        lean = [[0.25 * (q6[i + 1][c] - q6[i - 1][c]) for c in range(4)] for i in range(1, 5)]
        flux = []
        for i in range(1, 4):
            left = [q6[i][c] + lean[i - 1][c] for c in range(4)]
            right = [q6[i + 1][c] - lean[i][c] for c in range(4)]
            flux.append(interface(left, right, 1 + face // 2))
        for i in range(2):
            depth = depths[i + 2]
            where = depth if face % 2 == 0 else 31 - depth
            for c in range(4):
                extra = flux[i + 1][c] - flux[i][c]
                if face < 2:
                    spot = pl.ds(32 * where + 8 * j, 8)
                else:
                    spot = pl.ds(256 * j + where, 8, stride=32)
                fresh[c, spot, :] = fresh[c, spot, :] - ratio * extra

    copies = []
    for j in range(4):

        def update(n, carry):
            spot = pl.ds(pl.multiple_of(256 * j + 32 * n, 32), 32)
            for c in range(4):
                fresh[c, spot, :] = cells[c, spot, :] - ratio * inside[c, spot, :]
            return carry

        lax.fori_loop(0, 8, update, 0, unroll=True)
        for face in (2, 3):
            border(face, j)
        if j == 0 or j == 3:
            for piece in range(4):
                border(j // 3, piece)
        part = pl.ds(256 * j, 256)
        copies.append(pltpu.make_async_copy(fresh.at[:, part], out.at[:, part], out_sems.at[j]))
        copies[-1].start()
    for copy in copies:
        copy.wait()


def advance(*operands):
    return pl.pallas_call(
        step_kernel,
        out_shape=(
            jax.ShapeDtypeStruct((4, 1024, 128), F32),
            jax.ShapeDtypeStruct((1, 1), F32),
        ),
        in_specs=[VMEM] * 15,
        out_specs=(ANY, VMEM),
        scratch_shapes=[
            pltpu.VMEM((4, 1024, 128), F32),
            pltpu.VMEM((16 * 2 * 32, 128), F32),
            pltpu.VMEM((PACK, 128), F32),
            pltpu.VMEM((16 * 40, 128), F32),
            pltpu.VMEM((16 * 32, 128), F32),
            pltpu.SemaphoreType.DMA((4,)),
        ],
        compiler_params=pltpu.CompilerParams(vmem_limit_bytes=18 << 20),
        name="advance",
    )(*operands)


def two_way(array, chips):
    n = lax.axis_size(AXES)
    pairs = [(i, (i + (2 * chips if i % 2 == 0 else -2 * chips)) % n) for i in range(n)]
    return lax.ppermute(array, AXES, pairs)


def swap_cores(array):
    return lax.ppermute(array, AXES, [(i, i ^ 1) for i in range(lax.axis_size(AXES))])


def cross(array):
    n = lax.axis_size(AXES)
    return lax.ppermute(array, AXES, [(i, (i + (-3 if i % 2 else 3)) % n) for i in range(n)])


def compute(fields, patch_level, relation, face_half, neighbour, send_list):
    level = patch_level.reshape(1, 128)
    flat = fields.reshape(4, 1024, 128)
    own, swap, rows, deep = pack(flat, level, send_list[0].T)
    w = swap_cores(swap)

    def blk(array, n, count=1):
        return array[n * T : (n + count) * T]

    def ahead(j):
        return blk(own, j - 2)

    def beside(j):
        return blk(w, j - 1)

    low = jnp.minimum(swap[9 * T :], w[9 * T :])
    r4 = two_way(jnp.concatenate([ahead(8), beside(7), low]), 4)
    inside = inner(flat)
    low = jnp.minimum(low, r4[2 * T :])
    r3 = two_way(jnp.concatenate([ahead(6), beside(5), beside(8), low]), 3)
    r2 = two_way(jnp.concatenate([ahead(4), beside(3), ahead(7), beside(6), low]), 2)
    r1 = two_way(jnp.concatenate([ahead(2), beside(1), ahead(5), beside(4), low]), 1)
    q = cross(
        jnp.concatenate([ahead(3), beside(2), blk(r1, 2, 2), blk(r2, 2, 2), blk(r3, 2)])
    )
    depth = lax.axis_size("patch_2")
    columns = lax.axis_size(("patch_0", "patch_1"))
    low = jnp.minimum(jnp.minimum(low, r1[4 * T :]), jnp.minimum(r2[4 * T :], r3[3 * T :]))
    least = jnp.broadcast_to(low[0, :1], (2 * columns, 128))
    groups = [
        [(r * depth + (g + c) % depth) * 2 + c for r in range(columns) for c in range(2)]
        for g in range(depth)
    ]
    got = lax.all_to_all(least, AXES, 0, 0, tiled=True, axis_index_groups=groups)
    advanced, step = advance(
        flat, inside, rows, deep, r1, r2, r3, r4, w, q, got, level, relation.T, face_half.T,
        neighbour.transpose(1, 2, 0).reshape(8, 128),
    )
    return advanced.reshape(fields.shape), step[0, 0]


def stepper(mesh):
    split = Mesh(mesh.devices.reshape(SHAPE), AXES)
    return jax.shard_map(
        compute,
        mesh=split,
        in_specs=(
            P(None, None, None, AXES),
            P(AXES),
            P(AXES, None),
            P(AXES, None),
            P(AXES, None, None),
            P(AXES, None, None),
        ),
        out_specs=(P(None, None, None, AXES), P()),
        check_vma=False,
    )


def solution(mesh):
    return stepper(mesh)
```

```python
import jax
import jax.numpy as jnp
from jax import lax
from jax.experimental import pallas as pl
from jax.experimental.pallas import tpu as pltpu
from jax.sharding import Mesh
from jax.sharding import PartitionSpec as P

AXES = ("patch_0", "patch_1", "patch_2", "patch_3")
SHAPE = (4, 4, 16, 2)
COURANT = 0.4
CHUNKS = 8
NEAR = 64
ROWS = 80
PACK = 16 * ROWS
DEEP = 2 * 4 * 2 * 32
T = PACK // 128
LINE = 36
SPAN = 1160
F32 = jnp.float32
VMEM = pl.BlockSpec(memory_space=pltpu.VMEM)
ANY = pl.BlockSpec(memory_space=pl.ANY)


def spacing_of(level):
    return jnp.where(level == 6, 1.0, jnp.where(level == 5, 2.0, 4.0)).astype(F32)


def start_chunks(source, target, sems):
    width = 1024 // CHUNKS
    copies = []
    for chunk in range(CHUNKS):
        part = pl.ds(chunk * width, width)
        copies.append(pltpu.make_async_copy(source.at[:, part], target.at[:, part], sems.at[chunk]))
        copies[-1].start()
    return copies


def core_index():
    return lax.axis_index("patch_3")


def pack_kernel(fields, level_in, send_in, own, swap, rows, deep, cells, level, send, sems, small):
    extras = [
        pltpu.make_async_copy(level_in, level, small.at[0]),
        pltpu.make_async_copy(send_in, send, small.at[1]),
    ]
    copies = start_chunks(fields, cells, sems)
    for extra in extras:
        extra.start()
    width = 32 // CHUNKS
    fastest = jnp.zeros((32, 128), F32)
    for chunk in range(CHUNKS):
        copies[chunk].wait()

        def speeds(x, best):
            h, m, n = [cells[c, pl.ds(pl.multiple_of(32 * x, 32), 32), :] for c in range(3)]
            v = jnp.maximum(jnp.abs(m), jnp.abs(n)) / h
            return jnp.maximum(best, v + jnp.sqrt(h))

        fastest = lax.fori_loop(chunk * width, (chunk + 1) * width, speeds, fastest, unroll=True)
    for extra in extras:
        extra.wait()
    top = jnp.max(fastest, axis=0, keepdims=True)
    ratio = spacing_of(level[...]) / top
    swap[9 * T] = jnp.broadcast_to(jnp.min(ratio, axis=1, keepdims=True), (8, 128))

    for face in range(4):
        for c in range(4):
            base = (face * 4 + c) * ROWS
            at = [k if face % 2 == 0 else 31 - k for k in range(4)]
            inner = ((face - 2) * 4 + c) * 64
            for k in range(4):
                if face < 2 and k < 2:
                    rows[pl.ds(base + 32 * k, 32), :] = cells[c, pl.ds(32 * at[k], 32), :]
                if face >= 2:
                    line = cells[c, pl.ds(at[k], 32, stride=32), :]
                    if k < 2:
                        rows[pl.ds(base + 32 * k, 32), :] = line
                    else:
                        deep[pl.ds(inner + 32 * (k - 2), 32), :] = line

            def take(k, odd):
                if face < 2:
                    return cells[c, pl.ds(at[k] * 32 + odd, 16, stride=2), :]
                return deep[pl.ds(inner + 32 * (k - 2) + odd, 16, stride=2), :]

            total = take(2, 0) + take(3, 0)
            total = total + take(2, 1)
            total = total + take(3, 1)
            rows[pl.ds(base + NEAR, 16), :] = 0.25 * total

    lane = lax.broadcasted_iota(jnp.int32, (16, 128), 1)
    block = lax.broadcasted_iota(jnp.int32, (16, 128), 0)
    spread = jnp.where(((lane // 8) ^ (8 * core_index())) == block, 1.0, 0.0).astype(F32)
    listed = jnp.dot(send[...].astype(F32), spread, preferred_element_type=F32)
    slot = lax.broadcasted_iota(jnp.int32, (8, 128), 0)
    mine = (lax.broadcasted_iota(jnp.int32, (8, 128), 1) % 8) == slot
    chosen = jnp.sum(jnp.where(mine, listed, 0.0), axis=0, keepdims=True).astype(jnp.int32)
    index = jnp.broadcast_to(chosen, (128, 128))
    for tile in range(T):
        picked = jnp.take_along_axis(rows[pl.ds(tile * 128, 128), :], index, axis=1)
        turned = picked.T
        swap[8 * T + tile] = turned[0:8]
        for j in range(1, 8):
            own[(j - 1) * T + tile] = turned[8 * j : 8 * j + 8]
        for j in range(8):
            swap[j * T + tile] = turned[64 + 8 * j : 72 + 8 * j]


def tiles(n):
    return jax.ShapeDtypeStruct((n, 8, 128), F32)


def pack(fields, level, send):
    return pl.pallas_call(
        pack_kernel,
        out_shape=(
            tiles(7 * T),
            tiles(9 * T + 1),
            jax.ShapeDtypeStruct((PACK, 128), F32),
            jax.ShapeDtypeStruct((DEEP, 128), F32),
        ),
        in_specs=[pl.BlockSpec(memory_space=pltpu.HBM)] * 3,
        out_specs=(VMEM,) * 4,
        scratch_shapes=[
            pltpu.VMEM((4, 1024, 128), F32),
            pltpu.VMEM((1, 128), jnp.int32),
            pltpu.VMEM((8, 16), jnp.int32),
            pltpu.SemaphoreType.DMA((CHUNKS,)),
            pltpu.SemaphoreType.DMA((2,)),
        ],
        compiler_params=pltpu.CompilerParams(vmem_limit_bytes=8 << 20),
        name="pack",
    )(*[pltpu.with_memory_space_constraint(a, pltpu.HBM) for a in (fields, level, send)])


def physical(q, normal):
    h = q[0]
    m = q[normal]
    v = m / h
    flux = [m, q[1] * v, q[2] * v, q[3] * v]
    flux[normal] = flux[normal] + 0.5 * h * h
    return flux, jnp.abs(v) + jnp.sqrt(h)


def interface(left, right, normal):
    lf, ls = physical(left, normal)
    rf, rs = physical(right, normal)
    widest = 0.5 * jnp.maximum(ls, rs)
    return [0.5 * (lf[c] + rf[c]) - widest * (right[c] - left[c]) for c in range(4)]


def inner_kernel(cells, out, lines, fluxes):
    def lay(x, carry):
        for c in range(4):
            line = cells[c, pl.ds(pl.multiple_of(32 * x, 32), 32), :]
            lines[pl.ds(c * SPAN + x * LINE + 2, 32), :] = line
        return carry

    lax.fori_loop(0, 32, lay, 0, unroll=4)

    def along_y(n, carry):
        r = 1 + 8 * n
        left, right = [], []
        for c in range(4):
            before, here, after, beyond = [
                lines[pl.ds(c * SPAN + r + d, 8), :] for d in (-1, 0, 1, 2)
            ]
            left.append(here + 0.25 * (after - before))
            right.append(after - 0.25 * (beyond - here))
        flux = interface(left, right, 2)
        for c in range(4):
            fluxes[pl.ds(c * SPAN + r, 8), :] = flux[c]
        return carry

    lax.fori_loop(0, 144, along_y, 0, unroll=4)

    sub = lax.broadcasted_iota(jnp.int32, (8, 128), 0)
    for part in range(4):
        y = 8 * part

        def load(x):
            return [cells[c, pl.ds(pl.multiple_of(32 * x + y, 8), 8), :] for c in range(4)]

        def across(c, x):
            at = c * SPAN + x * LINE + y
            change = fluxes[pl.ds(at + 2, 8), :] - fluxes[pl.ds(at + 1, 8), :]
            if part == 0:
                change = jnp.where(sub >= 2, change, 0.0)
            if part == 3:
                change = jnp.where(sub < 6, change, 0.0)
            return change

        def store(c, x, value):
            out[c, pl.ds(pl.multiple_of(32 * x + y, 8), 8), :] = value

        def along_x(x, carry):
            here, ahead, left, last = carry
            beyond = load(x + 2)
            lean = [0.25 * (beyond[c] - here[c]) for c in range(4)]
            right = [ahead[c] - lean[c] for c in range(4)]
            flux = interface(left, right, 1)
            if last is not None:
                for c in range(4):
                    store(c, x, (flux[c] - last[c]) + across(c, x))
            return ahead, beyond, [ahead[c] + lean[c] for c in range(4)], flux

        first, second, third = load(0), load(1), load(2)
        left = [second[c] + 0.25 * (third[c] - first[c]) for c in range(4)]
        state = along_x(1, (second, third, left, None))
        lax.fori_loop(2, 30, along_x, state, unroll=4)
        for x in (0, 1, 30, 31):
            for c in range(4):
                store(c, x, across(c, x))


def inner(fields):
    return pl.pallas_call(
        inner_kernel,
        out_shape=jax.ShapeDtypeStruct((4, 1024, 128), F32),
        in_specs=[VMEM],
        out_specs=VMEM,
        scratch_shapes=[pltpu.VMEM((4 * SPAN, 128), F32), pltpu.VMEM((4 * SPAN, 128), F32)],
        compiler_params=pltpu.CompilerParams(vmem_limit_bytes=14 << 20),
        name="inner",
    )(fields)


def step_kernel(
    cells, inside, rows, deep, r1, r2, r3, r4, w, q, got, level, relation, half, refs,
    out, step, fresh, ghosts, pool, edge, weave, out_sems,
):
    sources = [
        (r1, T), (r1, 0), (r2, T), (r2, 0), (r3, T), (r3, 0), (r4, T), (r4, 0),
        (w, 8 * T), (q, T), (q, 0), (q, 3 * T), (q, 2 * T), (q, 5 * T), (q, 4 * T), (q, 6 * T),
    ]
    for tile in range(T):
        joined = jnp.concatenate([ref[at + tile] for ref, at in sources], axis=0)
        pool[pl.ds(tile * 128, 128), :] = joined.T

    flip = 64 * core_index()
    for face in range(4):
        kind = relation[pl.ds(face, 1), :]
        upper = half[pl.ds(face, 1), :] == 1
        names = [refs[pl.ds(2 * face + m, 1), :] for m in range(2)]
        away = [name >= 128 for name in names]
        local = [name & 127 for name in names]
        remote = [(name & 127) ^ flip for name in names]

        def gather(own_rows, pool_rows, m):
            shape = own_rows.shape
            a = jnp.take_along_axis(own_rows, jnp.broadcast_to(local[m], shape), axis=1)
            b = jnp.take_along_axis(pool_rows, jnp.broadcast_to(remote[m], shape), axis=1)
            return jnp.where(away[m], b, a)

        for c in range(4):
            base = ((face ^ 1) * 4 + c) * ROWS

            def coarse_first(ref):
                total = ref[pl.ds(base, 16, stride=2), :] + ref[pl.ds(base + 32, 16, stride=2), :]
                total = total + ref[pl.ds(base + 1, 16, stride=2), :]
                total = total + ref[pl.ds(base + 33, 16, stride=2), :]
                return 0.25 * total

            near = gather(rows[pl.ds(base, NEAR), :], pool[pl.ds(base, NEAR), :], 0)
            pairs = [
                (coarse_first(rows), coarse_first(pool)),
                (rows[pl.ds(base + NEAR, 16), :], pool[pl.ds(base + NEAR, 16), :]),
            ]
            column = near[0:32]
            spot = 40 * (4 * face + c)
            edge[pl.ds(spot + 1, 32), :] = column
            edge[pl.ds(spot, 1), :] = column[0:1]
            edge[pl.ds(spot + 33, 1), :] = column[31:32]
            slope = edge[pl.ds(spot + 2, 32), :] - edge[pl.ds(spot, 32), :]
            value = jnp.where(upper, column[16:32], column[0:16])
            tilt = 0.125 * jnp.where(upper, slope[16:32], slope[0:16])
            turn = 32 * (4 * face + c)
            weave[pl.ds(turn, 16, stride=2), :] = value - tilt
            weave[pl.ds(turn + 1, 16, stride=2), :] = value + tilt
            coarse = weave[pl.ds(turn, 32), :]
            sign = -1.0 if c == 1 + face // 2 else 1.0
            for g in range(2):
                fine = jnp.concatenate([gather(*pairs[g], 0), gather(*pairs[g], 1)], axis=0)
                mirror = sign * rows[pl.ds((face * 4 + c) * ROWS + 32 * g, 32), :]
                ghosts[pl.ds(((face * 4 + c) * 2 + g) * 32, 32), :] = jnp.where(
                    kind == 0,
                    mirror,
                    jnp.where(
                        kind == 1,
                        near[32 * g : 32 * g + 32],
                        jnp.where(kind == 2, coarse, fine),
                    ),
                )

    low = jnp.min(jnp.min(got[...], axis=0, keepdims=True), axis=1, keepdims=True)
    chosen = COURANT * low
    step[...] = chosen
    ratio = chosen / spacing_of(level[...])

    def border(face, j):
        def part(c, depth):
            if depth < 0:
                return ghosts[pl.ds(((face * 4 + c) * 2 - depth - 1) * 32 + 8 * j, 8), :]
            if face < 2:
                x = depth if face == 0 else 31 - depth
                return cells[c, pl.ds(32 * x + 8 * j, 8), :]
            if depth < 2:
                return rows[pl.ds((face * 4 + c) * ROWS + 32 * depth + 8 * j, 8), :]
            return deep[pl.ds(((face - 2) * 4 + c) * 64 + 32 * (depth - 2) + 8 * j, 8), :]

        depths = [-2, -1, 0, 1, 2, 3]
        if face % 2 == 1:
            depths = depths[::-1]
        q6 = [[part(c, depth) for c in range(4)] for depth in depths]
        lean = [[0.25 * (q6[i + 1][c] - q6[i - 1][c]) for c in range(4)] for i in range(1, 5)]
        flux = []
        for i in range(1, 4):
            left = [q6[i][c] + lean[i - 1][c] for c in range(4)]
            right = [q6[i + 1][c] - lean[i][c] for c in range(4)]
            flux.append(interface(left, right, 1 + face // 2))
        for i in range(2):
            depth = depths[i + 2]
            where = depth if face % 2 == 0 else 31 - depth
            for c in range(4):
                extra = flux[i + 1][c] - flux[i][c]
                if face < 2:
                    spot = pl.ds(32 * where + 8 * j, 8)
                else:
                    spot = pl.ds(256 * j + where, 8, stride=32)
                fresh[c, spot, :] = fresh[c, spot, :] - ratio * extra

    copies = []
    for j in range(4):

        def update(n, carry):
            spot = pl.ds(pl.multiple_of(256 * j + 32 * n, 32), 32)
            for c in range(4):
                fresh[c, spot, :] = cells[c, spot, :] - ratio * inside[c, spot, :]
            return carry

        lax.fori_loop(0, 8, update, 0, unroll=True)
        for face in (2, 3):
            border(face, j)
        if j == 0 or j == 3:
            for piece in range(4):
                border(j // 3, piece)
        part = pl.ds(256 * j, 256)
        copies.append(pltpu.make_async_copy(fresh.at[:, part], out.at[:, part], out_sems.at[j]))
        copies[-1].start()
    for copy in copies:
        copy.wait()


def advance(*operands):
    return pl.pallas_call(
        step_kernel,
        out_shape=(
            jax.ShapeDtypeStruct((4, 1024, 128), F32),
            jax.ShapeDtypeStruct((1, 1), F32),
        ),
        in_specs=[VMEM] * 15,
        out_specs=(ANY, VMEM),
        scratch_shapes=[
            pltpu.VMEM((4, 1024, 128), F32),
            pltpu.VMEM((16 * 2 * 32, 128), F32),
            pltpu.VMEM((PACK, 128), F32),
            pltpu.VMEM((16 * 40, 128), F32),
            pltpu.VMEM((16 * 32, 128), F32),
            pltpu.SemaphoreType.DMA((4,)),
        ],
        compiler_params=pltpu.CompilerParams(vmem_limit_bytes=18 << 20),
        name="advance",
    )(*operands)


def two_way(array, chips):
    n = lax.axis_size(AXES)
    pairs = [(i, (i + (2 * chips if i % 2 == 0 else -2 * chips)) % n) for i in range(n)]
    return lax.ppermute(array, AXES, pairs)


def swap_cores(array):
    return lax.ppermute(array, AXES, [(i, i ^ 1) for i in range(lax.axis_size(AXES))])


def cross(array):
    n = lax.axis_size(AXES)
    return lax.ppermute(array, AXES, [(i, (i + (-3 if i % 2 else 3)) % n) for i in range(n)])


def compute(fields, patch_level, relation, face_half, neighbour, send_list):
    level = patch_level.reshape(1, 128)
    flat = fields.reshape(4, 1024, 128)
    own, swap, rows, deep = pack(flat, level, send_list[0].T)
    w = swap_cores(swap)

    def blk(array, n, count=1):
        return array[n * T : (n + count) * T]

    def ahead(j):
        return blk(own, j - 2)

    def beside(j):
        return blk(w, j - 1)

    low = jnp.minimum(swap[9 * T :], w[9 * T :])
    r3 = two_way(jnp.concatenate([ahead(6), beside(5), beside(8), low]), 3)
    r2 = two_way(jnp.concatenate([ahead(4), beside(3), ahead(7), beside(6), low]), 2)
    r1 = two_way(jnp.concatenate([ahead(2), beside(1), ahead(5), beside(4), low]), 1)
    r4 = two_way(jnp.concatenate([ahead(8), beside(7)]), 4)
    low = jnp.minimum(jnp.minimum(low, r1[4 * T :]), jnp.minimum(r2[4 * T :], r3[3 * T :]))
    beyond = two_way(low, 4)
    q = cross(
        jnp.concatenate([ahead(3), beside(2), blk(r1, 2, 2), blk(r2, 2, 2), blk(r3, 2)])
    )
    inside = inner(flat)
    depth = lax.axis_size("patch_2")
    columns = lax.axis_size(("patch_0", "patch_1"))
    low = jnp.minimum(low, beyond)
    least = jnp.broadcast_to(low[0, :1], (2 * columns, 128))
    groups = [
        [(r * depth + (g + c) % depth) * 2 + c for r in range(columns) for c in range(2)]
        for g in range(depth)
    ]
    least, r4 = lax.optimization_barrier((least, r4))
    got = lax.all_to_all(least, AXES, 0, 0, tiled=True, axis_index_groups=groups)
    advanced, step = advance(
        flat, inside, rows, deep, r1, r2, r3, r4, w, q, got, level, relation.T, face_half.T,
        neighbour.transpose(1, 2, 0).reshape(8, 128),
    )
    return advanced.reshape(fields.shape), step[0, 0]


def stepper(mesh):
    split = Mesh(mesh.devices.reshape(SHAPE), AXES)
    return jax.shard_map(
        compute,
        mesh=split,
        in_specs=(
            P(None, None, None, AXES),
            P(AXES),
            P(AXES, None),
            P(AXES, None),
            P(AXES, None, None),
            P(AXES, None, None),
        ),
        out_specs=(P(None, None, None, AXES), P()),
        check_vma=False,
    )


def solution(mesh):
    return stepper(mesh)
```

```python
import jax
import jax.numpy as jnp
from jax import lax
from jax.experimental import pallas as pl
from jax.experimental.pallas import tpu as pltpu
from jax.sharding import Mesh
from jax.sharding import PartitionSpec as P

AXES = ("patch_0", "patch_1", "patch_2", "patch_3")
SHAPE = (4, 4, 16, 2)
COURANT = 0.4
CHUNKS = 8
NEAR = 64
ROWS = 80
PACK = 16 * ROWS
DEEP = 2 * 4 * 2 * 32
T = PACK // 128
LINE = 36
SPAN = 1160
F32 = jnp.float32
VMEM = pl.BlockSpec(memory_space=pltpu.VMEM)
ANY = pl.BlockSpec(memory_space=pl.ANY)


def spacing_of(level):
    return jnp.where(level == 6, 1.0, jnp.where(level == 5, 2.0, 4.0)).astype(F32)


def start_chunks(source, target, sems):
    width = 1024 // CHUNKS
    copies = []
    for chunk in range(CHUNKS):
        part = pl.ds(chunk * width, width)
        copies.append(pltpu.make_async_copy(source.at[:, part], target.at[:, part], sems.at[chunk]))
        copies[-1].start()
    return copies


def core_index():
    return lax.axis_index("patch_3")


def pack_kernel(fields, level_in, send_in, own, swap, rows, deep, cells, level, send, sems, small):
    extras = [
        pltpu.make_async_copy(level_in, level, small.at[0]),
        pltpu.make_async_copy(send_in, send, small.at[1]),
    ]
    copies = start_chunks(fields, cells, sems)
    for extra in extras:
        extra.start()
    width = 32 // CHUNKS
    fastest = jnp.zeros((32, 128), F32)
    for chunk in range(CHUNKS):
        copies[chunk].wait()

        def speeds(x, best):
            h, m, n = [cells[c, pl.ds(pl.multiple_of(32 * x, 32), 32), :] for c in range(3)]
            root = lax.rsqrt(h)
            v = jnp.maximum(jnp.abs(m), jnp.abs(n)) * (root * root)
            return jnp.maximum(best, v + h * root)

        fastest = lax.fori_loop(chunk * width, (chunk + 1) * width, speeds, fastest, unroll=True)
    for extra in extras:
        extra.wait()
    top = jnp.max(fastest, axis=0, keepdims=True)
    ratio = spacing_of(level[...]) / top
    swap[9 * T] = jnp.broadcast_to(jnp.min(ratio, axis=1, keepdims=True), (8, 128))

    for face in range(4):
        for c in range(4):
            base = (face * 4 + c) * ROWS
            at = [k if face % 2 == 0 else 31 - k for k in range(4)]
            inner = ((face - 2) * 4 + c) * 64
            for k in range(4):
                if face < 2 and k < 2:
                    rows[pl.ds(base + 32 * k, 32), :] = cells[c, pl.ds(32 * at[k], 32), :]
                if face >= 2:
                    line = cells[c, pl.ds(at[k], 32, stride=32), :]
                    if k < 2:
                        rows[pl.ds(base + 32 * k, 32), :] = line
                    else:
                        deep[pl.ds(inner + 32 * (k - 2), 32), :] = line

            def take(k, odd):
                if face < 2:
                    return cells[c, pl.ds(at[k] * 32 + odd, 16, stride=2), :]
                return deep[pl.ds(inner + 32 * (k - 2) + odd, 16, stride=2), :]

            total = take(2, 0) + take(3, 0)
            total = total + take(2, 1)
            total = total + take(3, 1)
            rows[pl.ds(base + NEAR, 16), :] = 0.25 * total

    lane = lax.broadcasted_iota(jnp.int32, (16, 128), 1)
    block = lax.broadcasted_iota(jnp.int32, (16, 128), 0)
    spread = jnp.where(((lane // 8) ^ (8 * core_index())) == block, 1.0, 0.0).astype(F32)
    listed = jnp.dot(send[...].astype(F32), spread, preferred_element_type=F32)
    slot = lax.broadcasted_iota(jnp.int32, (8, 128), 0)
    mine = (lax.broadcasted_iota(jnp.int32, (8, 128), 1) % 8) == slot
    chosen = jnp.sum(jnp.where(mine, listed, 0.0), axis=0, keepdims=True).astype(jnp.int32)
    index = jnp.broadcast_to(chosen, (128, 128))
    for tile in range(T):
        picked = jnp.take_along_axis(rows[pl.ds(tile * 128, 128), :], index, axis=1)
        turned = picked.T
        swap[8 * T + tile] = turned[0:8]
        for j in range(1, 8):
            own[(j - 1) * T + tile] = turned[8 * j : 8 * j + 8]
        for j in range(8):
            swap[j * T + tile] = turned[64 + 8 * j : 72 + 8 * j]


def tiles(n):
    return jax.ShapeDtypeStruct((n, 8, 128), F32)


def pack(fields, level, send):
    return pl.pallas_call(
        pack_kernel,
        out_shape=(
            tiles(7 * T),
            tiles(9 * T + 1),
            jax.ShapeDtypeStruct((PACK, 128), F32),
            jax.ShapeDtypeStruct((DEEP, 128), F32),
        ),
        in_specs=[pl.BlockSpec(memory_space=pltpu.HBM)] * 3,
        out_specs=(VMEM,) * 4,
        scratch_shapes=[
            pltpu.VMEM((4, 1024, 128), F32),
            pltpu.VMEM((1, 128), jnp.int32),
            pltpu.VMEM((8, 16), jnp.int32),
            pltpu.SemaphoreType.DMA((CHUNKS,)),
            pltpu.SemaphoreType.DMA((2,)),
        ],
        compiler_params=pltpu.CompilerParams(vmem_limit_bytes=8 << 20),
        name="pack",
    )(*[pltpu.with_memory_space_constraint(a, pltpu.HBM) for a in (fields, level, send)])


def physical(q, normal):
    h = q[0]
    m = q[normal]
    root = lax.rsqrt(h)
    v = m * (root * root)
    flux = [m, q[1] * v, q[2] * v, q[3] * v]
    flux[normal] = flux[normal] + 0.5 * h * h
    return flux, jnp.abs(v) + h * root


def interface(left, right, normal):
    lf, ls = physical(left, normal)
    rf, rs = physical(right, normal)
    widest = jnp.maximum(ls, rs)
    return [(lf[c] + rf[c]) - widest * (right[c] - left[c]) for c in range(4)]


def inner_kernel(cells, out, lines, fluxes):
    def lay(x, carry):
        for c in range(4):
            line = cells[c, pl.ds(pl.multiple_of(32 * x, 32), 32), :]
            lines[pl.ds(c * SPAN + x * LINE + 2, 32), :] = line
        return carry

    lax.fori_loop(0, 32, lay, 0, unroll=4)

    def along_y(n, carry):
        r = 1 + 8 * n
        left, right = [], []
        for c in range(4):
            before, here, after, beyond = [
                lines[pl.ds(c * SPAN + r + d, 8), :] for d in (-1, 0, 1, 2)
            ]
            left.append(here + 0.25 * (after - before))
            right.append(after - 0.25 * (beyond - here))
        flux = interface(left, right, 2)
        for c in range(4):
            fluxes[pl.ds(c * SPAN + r, 8), :] = flux[c]
        return carry

    lax.fori_loop(0, 144, along_y, 0, unroll=4)

    sub = lax.broadcasted_iota(jnp.int32, (8, 128), 0)
    for part in range(4):
        y = 8 * part

        def load(x):
            return [cells[c, pl.ds(pl.multiple_of(32 * x + y, 8), 8), :] for c in range(4)]

        def across(c, x):
            at = c * SPAN + x * LINE + y
            change = fluxes[pl.ds(at + 2, 8), :] - fluxes[pl.ds(at + 1, 8), :]
            if part == 0:
                change = jnp.where(sub >= 2, change, 0.0)
            if part == 3:
                change = jnp.where(sub < 6, change, 0.0)
            return change

        def store(c, x, value):
            out[c, pl.ds(pl.multiple_of(32 * x + y, 8), 8), :] = value

        def along_x(x, carry):
            here, ahead, left, last = carry
            beyond = load(x + 2)
            lean = [0.25 * (beyond[c] - here[c]) for c in range(4)]
            right = [ahead[c] - lean[c] for c in range(4)]
            flux = interface(left, right, 1)
            if last is not None:
                for c in range(4):
                    store(c, x, (flux[c] - last[c]) + across(c, x))
            return ahead, beyond, [ahead[c] + lean[c] for c in range(4)], flux

        first, second, third = load(0), load(1), load(2)
        left = [second[c] + 0.25 * (third[c] - first[c]) for c in range(4)]
        state = along_x(1, (second, third, left, None))
        lax.fori_loop(2, 30, along_x, state, unroll=4)
        for x in (0, 1, 30, 31):
            for c in range(4):
                store(c, x, across(c, x))


def inner(fields):
    return pl.pallas_call(
        inner_kernel,
        out_shape=jax.ShapeDtypeStruct((4, 1024, 128), F32),
        in_specs=[VMEM],
        out_specs=VMEM,
        scratch_shapes=[pltpu.VMEM((4 * SPAN, 128), F32), pltpu.VMEM((4 * SPAN, 128), F32)],
        compiler_params=pltpu.CompilerParams(vmem_limit_bytes=14 << 20),
        name="inner",
    )(fields)


def step_kernel(
    cells, inside, rows, deep, r1, r2, r3, r4, w, q, got, level, relation, half, refs,
    out, step, fresh, ghosts, pool, edge, weave, out_sems,
):
    sources = [
        (r1, T), (r1, 0), (r2, T), (r2, 0), (r3, T), (r3, 0), (r4, T), (r4, 0),
        (w, 8 * T), (q, T), (q, 0), (q, 3 * T), (q, 2 * T), (q, 5 * T), (q, 4 * T), (q, 6 * T),
    ]
    for tile in range(T):
        joined = jnp.concatenate([ref[at + tile] for ref, at in sources], axis=0)
        pool[pl.ds(tile * 128, 128), :] = joined.T

    flip = 64 * core_index()
    for face in range(4):
        kind = relation[pl.ds(face, 1), :]
        upper = half[pl.ds(face, 1), :] == 1
        names = [refs[pl.ds(2 * face + m, 1), :] for m in range(2)]
        away = [name >= 128 for name in names]
        local = [name & 127 for name in names]
        remote = [(name & 127) ^ flip for name in names]

        def gather(own_rows, pool_rows, m):
            shape = own_rows.shape
            a = jnp.take_along_axis(own_rows, jnp.broadcast_to(local[m], shape), axis=1)
            b = jnp.take_along_axis(pool_rows, jnp.broadcast_to(remote[m], shape), axis=1)
            return jnp.where(away[m], b, a)

        for c in range(4):
            base = ((face ^ 1) * 4 + c) * ROWS

            def coarse_first(ref):
                total = ref[pl.ds(base, 16, stride=2), :] + ref[pl.ds(base + 32, 16, stride=2), :]
                total = total + ref[pl.ds(base + 1, 16, stride=2), :]
                total = total + ref[pl.ds(base + 33, 16, stride=2), :]
                return 0.25 * total

            near = gather(rows[pl.ds(base, NEAR), :], pool[pl.ds(base, NEAR), :], 0)
            pairs = [
                (coarse_first(rows), coarse_first(pool)),
                (rows[pl.ds(base + NEAR, 16), :], pool[pl.ds(base + NEAR, 16), :]),
            ]
            column = near[0:32]
            spot = 40 * (4 * face + c)
            edge[pl.ds(spot + 1, 32), :] = column
            edge[pl.ds(spot, 1), :] = column[0:1]
            edge[pl.ds(spot + 33, 1), :] = column[31:32]
            slope = edge[pl.ds(spot + 2, 32), :] - edge[pl.ds(spot, 32), :]
            value = jnp.where(upper, column[16:32], column[0:16])
            tilt = 0.125 * jnp.where(upper, slope[16:32], slope[0:16])
            turn = 32 * (4 * face + c)
            weave[pl.ds(turn, 16, stride=2), :] = value - tilt
            weave[pl.ds(turn + 1, 16, stride=2), :] = value + tilt
            coarse = weave[pl.ds(turn, 32), :]
            sign = -1.0 if c == 1 + face // 2 else 1.0
            for g in range(2):
                fine = jnp.concatenate([gather(*pairs[g], 0), gather(*pairs[g], 1)], axis=0)
                mirror = sign * rows[pl.ds((face * 4 + c) * ROWS + 32 * g, 32), :]
                ghosts[pl.ds(((face * 4 + c) * 2 + g) * 32, 32), :] = jnp.where(
                    kind == 0,
                    mirror,
                    jnp.where(
                        kind == 1,
                        near[32 * g : 32 * g + 32],
                        jnp.where(kind == 2, coarse, fine),
                    ),
                )

    low = jnp.min(jnp.min(got[...], axis=0, keepdims=True), axis=1, keepdims=True)
    chosen = COURANT * low
    step[...] = chosen
    ratio = (0.5 * chosen) / spacing_of(level[...])

    def border(face, j):
        def part(c, depth):
            if depth < 0:
                return ghosts[pl.ds(((face * 4 + c) * 2 - depth - 1) * 32 + 8 * j, 8), :]
            if face < 2:
                x = depth if face == 0 else 31 - depth
                return cells[c, pl.ds(32 * x + 8 * j, 8), :]
            if depth < 2:
                return rows[pl.ds((face * 4 + c) * ROWS + 32 * depth + 8 * j, 8), :]
            return deep[pl.ds(((face - 2) * 4 + c) * 64 + 32 * (depth - 2) + 8 * j, 8), :]

        depths = [-2, -1, 0, 1, 2, 3]
        if face % 2 == 1:
            depths = depths[::-1]
        q6 = [[part(c, depth) for c in range(4)] for depth in depths]
        lean = [[0.25 * (q6[i + 1][c] - q6[i - 1][c]) for c in range(4)] for i in range(1, 5)]
        flux = []
        for i in range(1, 4):
            left = [q6[i][c] + lean[i - 1][c] for c in range(4)]
            right = [q6[i + 1][c] - lean[i][c] for c in range(4)]
            flux.append(interface(left, right, 1 + face // 2))
        for i in range(2):
            depth = depths[i + 2]
            where = depth if face % 2 == 0 else 31 - depth
            for c in range(4):
                extra = flux[i + 1][c] - flux[i][c]
                if face < 2:
                    spot = pl.ds(32 * where + 8 * j, 8)
                else:
                    spot = pl.ds(256 * j + where, 8, stride=32)
                fresh[c, spot, :] = fresh[c, spot, :] - ratio * extra

    copies = []
    for j in range(4):

        def update(n, carry):
            spot = pl.ds(pl.multiple_of(256 * j + 32 * n, 32), 32)
            for c in range(4):
                fresh[c, spot, :] = cells[c, spot, :] - ratio * inside[c, spot, :]
            return carry

        lax.fori_loop(0, 8, update, 0, unroll=True)
        for face in (2, 3):
            border(face, j)
        if j == 0 or j == 3:
            for piece in range(4):
                border(j // 3, piece)
        part = pl.ds(256 * j, 256)
        copies.append(pltpu.make_async_copy(fresh.at[:, part], out.at[:, part], out_sems.at[j]))
        copies[-1].start()
    for copy in copies:
        copy.wait()


def advance(*operands):
    return pl.pallas_call(
        step_kernel,
        out_shape=(
            jax.ShapeDtypeStruct((4, 1024, 128), F32),
            jax.ShapeDtypeStruct((1, 1), F32),
        ),
        in_specs=[VMEM] * 15,
        out_specs=(ANY, VMEM),
        scratch_shapes=[
            pltpu.VMEM((4, 1024, 128), F32),
            pltpu.VMEM((16 * 2 * 32, 128), F32),
            pltpu.VMEM((PACK, 128), F32),
            pltpu.VMEM((16 * 40, 128), F32),
            pltpu.VMEM((16 * 32, 128), F32),
            pltpu.SemaphoreType.DMA((4,)),
        ],
        compiler_params=pltpu.CompilerParams(vmem_limit_bytes=18 << 20),
        name="advance",
    )(*operands)


def two_way(array, chips):
    n = lax.axis_size(AXES)
    pairs = [(i, (i + (2 * chips if i % 2 == 0 else -2 * chips)) % n) for i in range(n)]
    return lax.ppermute(array, AXES, pairs)


def swap_cores(array):
    return lax.ppermute(array, AXES, [(i, i ^ 1) for i in range(lax.axis_size(AXES))])


def cross(array):
    n = lax.axis_size(AXES)
    return lax.ppermute(array, AXES, [(i, (i + (-3 if i % 2 else 3)) % n) for i in range(n)])


def compute(fields, patch_level, relation, face_half, neighbour, send_list):
    level = patch_level.reshape(1, 128)
    flat = fields.reshape(4, 1024, 128)
    own, swap, rows, deep = pack(flat, level, send_list[0].T)
    w = swap_cores(swap)

    def blk(array, n, count=1):
        return array[n * T : (n + count) * T]

    def ahead(j):
        return blk(own, j - 2)

    def beside(j):
        return blk(w, j - 1)

    low = jnp.minimum(swap[9 * T :], w[9 * T :])
    r3 = two_way(jnp.concatenate([ahead(6), beside(5), beside(8), low]), 3)
    r2 = two_way(jnp.concatenate([ahead(4), beside(3), ahead(7), beside(6), low]), 2)
    r1 = two_way(jnp.concatenate([ahead(2), beside(1), ahead(5), beside(4), low]), 1)
    low = jnp.minimum(jnp.minimum(low, r1[4 * T :]), jnp.minimum(r2[4 * T :], r3[3 * T :]))
    r4 = two_way(jnp.concatenate([ahead(8), beside(7), low]), 4)
    q = cross(
        jnp.concatenate([ahead(3), beside(2), blk(r1, 2, 2), blk(r2, 2, 2), blk(r3, 2)])
    )
    inside = inner(flat)
    depth = lax.axis_size("patch_2")
    columns = lax.axis_size(("patch_0", "patch_1"))
    low = jnp.minimum(low, r4[2 * T :])
    least = jnp.broadcast_to(low[0, :1], (2 * columns, 128))
    groups = [
        [(r * depth + (g + c) % depth) * 2 + c for r in range(columns) for c in range(2)]
        for g in range(depth)
    ]
    got = lax.all_to_all(least, AXES, 0, 0, tiled=True, axis_index_groups=groups)
    advanced, step = advance(
        flat, inside, rows, deep, r1, r2, r3, r4, w, q, got, level, relation.T, face_half.T,
        neighbour.transpose(1, 2, 0).reshape(8, 128),
    )
    return advanced.reshape(fields.shape), step[0, 0]


def stepper(mesh):
    split = Mesh(mesh.devices.reshape(SHAPE), AXES)
    return jax.shard_map(
        compute,
        mesh=split,
        in_specs=(
            P(None, None, None, AXES),
            P(AXES),
            P(AXES, None),
            P(AXES, None),
            P(AXES, None, None),
            P(AXES, None, None),
        ),
        out_specs=(P(None, None, None, AXES), P()),
        check_vma=False,
    )


def solution(mesh):
    return stepper(mesh)
```

```python
import jax
import jax.numpy as jnp
from jax import lax
from jax.experimental import pallas as pl
from jax.experimental.pallas import tpu as pltpu
from jax.sharding import Mesh
from jax.sharding import PartitionSpec as P

AXES = ("patch_0", "patch_1", "patch_2", "patch_3")
SHAPE = (4, 4, 16, 2)
COURANT = 0.4
CHUNKS = 8
NEAR = 64
ROWS = 80
PACK = 16 * ROWS
DEEP = 2 * 4 * 2 * 32
T = PACK // 128
LINE = 36
SPAN = 1160
F32 = jnp.float32
VMEM = pl.BlockSpec(memory_space=pltpu.VMEM)
ANY = pl.BlockSpec(memory_space=pl.ANY)


def spacing_of(level):
    return jnp.where(level == 6, 1.0, jnp.where(level == 5, 2.0, 4.0)).astype(F32)


def start_chunks(source, target, sems):
    width = 1024 // CHUNKS
    copies = []
    for chunk in range(CHUNKS):
        part = pl.ds(chunk * width, width)
        copies.append(pltpu.make_async_copy(source.at[:, part], target.at[:, part], sems.at[chunk]))
        copies[-1].start()
    return copies


def core_index():
    return lax.axis_index("patch_3")


def pack_kernel(fields, level_in, send_in, own, swap, rows, deep, cells, level, send, sems, small):
    extras = [
        pltpu.make_async_copy(level_in, level, small.at[0]),
        pltpu.make_async_copy(send_in, send, small.at[1]),
    ]
    copies = start_chunks(fields, cells, sems)
    for extra in extras:
        extra.start()
    width = 32 // CHUNKS
    fastest = jnp.zeros((32, 128), F32)
    for chunk in range(CHUNKS):
        copies[chunk].wait()

        def speeds(x, best):
            h, m, n = [cells[c, pl.ds(pl.multiple_of(32 * x, 32), 32), :] for c in range(3)]
            root = lax.rsqrt(h)
            v = jnp.maximum(jnp.abs(m), jnp.abs(n)) * (root * root)
            return jnp.maximum(best, v + h * root)

        fastest = lax.fori_loop(chunk * width, (chunk + 1) * width, speeds, fastest, unroll=True)
    for extra in extras:
        extra.wait()
    top = jnp.max(fastest, axis=0, keepdims=True)
    ratio = spacing_of(level[...]) / top
    swap[9 * T] = jnp.broadcast_to(jnp.min(ratio, axis=1, keepdims=True), (8, 128))

    for face in range(4):
        for c in range(4):
            base = (face * 4 + c) * ROWS
            at = [k if face % 2 == 0 else 31 - k for k in range(4)]
            inner = ((face - 2) * 4 + c) * 64
            for k in range(4):
                if face < 2 and k < 2:
                    rows[pl.ds(base + 32 * k, 32), :] = cells[c, pl.ds(32 * at[k], 32), :]
                if face >= 2:
                    line = cells[c, pl.ds(at[k], 32, stride=32), :]
                    if k < 2:
                        rows[pl.ds(base + 32 * k, 32), :] = line
                    else:
                        deep[pl.ds(inner + 32 * (k - 2), 32), :] = line

            def take(k, odd):
                if face < 2:
                    return cells[c, pl.ds(at[k] * 32 + odd, 16, stride=2), :]
                return deep[pl.ds(inner + 32 * (k - 2) + odd, 16, stride=2), :]

            total = take(2, 0) + take(3, 0)
            total = total + take(2, 1)
            total = total + take(3, 1)
            rows[pl.ds(base + NEAR, 16), :] = 0.25 * total

    lane = lax.broadcasted_iota(jnp.int32, (16, 128), 1)
    block = lax.broadcasted_iota(jnp.int32, (16, 128), 0)
    spread = jnp.where(((lane // 8) ^ (8 * core_index())) == block, 1.0, 0.0).astype(F32)
    listed = jnp.dot(send[...].astype(F32), spread, preferred_element_type=F32)
    slot = lax.broadcasted_iota(jnp.int32, (8, 128), 0)
    mine = (lax.broadcasted_iota(jnp.int32, (8, 128), 1) % 8) == slot
    chosen = jnp.sum(jnp.where(mine, listed, 0.0), axis=0, keepdims=True).astype(jnp.int32)
    index = jnp.broadcast_to(chosen, (128, 128))
    for tile in range(T):
        picked = jnp.take_along_axis(rows[pl.ds(tile * 128, 128), :], index, axis=1)
        turned = picked.T
        swap[8 * T + tile] = turned[0:8]
        for j in range(1, 8):
            own[(j - 1) * T + tile] = turned[8 * j : 8 * j + 8]
        for j in range(8):
            swap[j * T + tile] = turned[64 + 8 * j : 72 + 8 * j]


def tiles(n):
    return jax.ShapeDtypeStruct((n, 8, 128), F32)


def pack(fields, level, send):
    return pl.pallas_call(
        pack_kernel,
        out_shape=(
            tiles(7 * T),
            tiles(9 * T + 1),
            jax.ShapeDtypeStruct((PACK, 128), F32),
            jax.ShapeDtypeStruct((DEEP, 128), F32),
        ),
        in_specs=[pl.BlockSpec(memory_space=pltpu.HBM)] * 3,
        out_specs=(VMEM,) * 4,
        scratch_shapes=[
            pltpu.VMEM((4, 1024, 128), F32),
            pltpu.VMEM((1, 128), jnp.int32),
            pltpu.VMEM((8, 16), jnp.int32),
            pltpu.SemaphoreType.DMA((CHUNKS,)),
            pltpu.SemaphoreType.DMA((2,)),
        ],
        compiler_params=pltpu.CompilerParams(vmem_limit_bytes=8 << 20),
        name="pack",
    )(*[pltpu.with_memory_space_constraint(a, pltpu.HBM) for a in (fields, level, send)])


def physical(q, normal):
    h = q[0]
    m = q[normal]
    root = lax.rsqrt(h)
    v = m * (root * root)
    flux = [m, q[1] * v, q[2] * v, q[3] * v]
    flux[normal] = flux[normal] + 0.5 * h * h
    return flux, jnp.abs(v) + h * root


def interface(left, right, normal):
    lf, ls = physical(left, normal)
    rf, rs = physical(right, normal)
    widest = jnp.maximum(ls, rs)
    return [(lf[c] + rf[c]) - widest * (right[c] - left[c]) for c in range(4)]


def candidates(source, index, kind, upper, base, edge, weave, slot):
    def take(piece, m):
        return jnp.take_along_axis(piece, jnp.broadcast_to(index[m], piece.shape), axis=1)

    near = take(source[pl.ds(base, NEAR), :], 0)
    first = source[pl.ds(base, 16, stride=2), :] + source[pl.ds(base + 32, 16, stride=2), :]
    first = first + source[pl.ds(base + 1, 16, stride=2), :]
    first = 0.25 * (first + source[pl.ds(base + 33, 16, stride=2), :])
    pieces = [first, source[pl.ds(base + NEAR, 16), :]]
    column = near[0:32]
    spot = 40 * slot
    edge[pl.ds(spot + 1, 32), :] = column
    edge[pl.ds(spot, 1), :] = column[0:1]
    edge[pl.ds(spot + 33, 1), :] = column[31:32]
    slope = edge[pl.ds(spot + 2, 32), :] - edge[pl.ds(spot, 32), :]
    value = jnp.where(upper, column[16:32], column[0:16])
    tilt = 0.125 * jnp.where(upper, slope[16:32], slope[0:16])
    turn = 32 * slot
    weave[pl.ds(turn, 16, stride=2), :] = value - tilt
    weave[pl.ds(turn + 1, 16, stride=2), :] = value + tilt
    coarse = weave[pl.ds(turn, 32), :]
    found = []
    for g in range(2):
        fine = jnp.concatenate([take(pieces[g], 0), take(pieces[g], 1)], axis=0)
        other = jnp.where(kind == 2, coarse, fine)
        found.append(jnp.where(kind == 1, near[32 * g : 32 * g + 32], other))
    return found


def inner_kernel(
    cells, rows, relation, half, refs, out, ghosts, lines, fluxes, edge, weave
):
    for face in range(4):
        kind = relation[pl.ds(face, 1), :]
        upper = half[pl.ds(face, 1), :] == 1
        index = [refs[pl.ds(2 * face + m, 1), :] & 127 for m in range(2)]
        for c in range(4):
            slot = 4 * face + c
            base = ((face ^ 1) * 4 + c) * ROWS
            found = candidates(rows, index, kind, upper, base, edge, weave, slot)
            sign = -1.0 if c == 1 + face // 2 else 1.0
            for g in range(2):
                mirror = sign * rows[pl.ds(slot * ROWS + 32 * g, 32), :]
                ghosts[pl.ds((slot * 2 + g) * 32, 32), :] = jnp.where(kind == 0, mirror, found[g])

    def lay(x, carry):
        for c in range(4):
            line = cells[c, pl.ds(pl.multiple_of(32 * x, 32), 32), :]
            lines[pl.ds(c * SPAN + x * LINE + 2, 32), :] = line
        return carry

    lax.fori_loop(0, 32, lay, 0, unroll=4)

    def along_y(n, carry):
        r = 1 + 8 * n
        left, right = [], []
        for c in range(4):
            before, here, after, beyond = [
                lines[pl.ds(c * SPAN + r + d, 8), :] for d in (-1, 0, 1, 2)
            ]
            left.append(here + 0.25 * (after - before))
            right.append(after - 0.25 * (beyond - here))
        flux = interface(left, right, 2)
        for c in range(4):
            fluxes[pl.ds(c * SPAN + r, 8), :] = flux[c]
        return carry

    lax.fori_loop(0, 144, along_y, 0, unroll=4)

    sub = lax.broadcasted_iota(jnp.int32, (8, 128), 0)
    for part in range(4):
        y = 8 * part

        def load(x):
            return [cells[c, pl.ds(pl.multiple_of(32 * x + y, 8), 8), :] for c in range(4)]

        def across(c, x):
            at = c * SPAN + x * LINE + y
            change = fluxes[pl.ds(at + 2, 8), :] - fluxes[pl.ds(at + 1, 8), :]
            if part == 0:
                change = jnp.where(sub >= 2, change, 0.0)
            if part == 3:
                change = jnp.where(sub < 6, change, 0.0)
            return change

        def store(c, x, value):
            out[c, pl.ds(pl.multiple_of(32 * x + y, 8), 8), :] = value

        def along_x(x, carry):
            here, ahead, left, last = carry
            beyond = load(x + 2)
            lean = [0.25 * (beyond[c] - here[c]) for c in range(4)]
            right = [ahead[c] - lean[c] for c in range(4)]
            flux = interface(left, right, 1)
            if last is not None:
                for c in range(4):
                    store(c, x, (flux[c] - last[c]) + across(c, x))
            return ahead, beyond, [ahead[c] + lean[c] for c in range(4)], flux

        first, second, third = load(0), load(1), load(2)
        left = [second[c] + 0.25 * (third[c] - first[c]) for c in range(4)]
        state = along_x(1, (second, third, left, None))
        lax.fori_loop(2, 30, along_x, state, unroll=4)
        for x in (0, 1, 30, 31):
            for c in range(4):
                store(c, x, across(c, x))


def inner(*operands):
    return pl.pallas_call(
        inner_kernel,
        out_shape=(
            jax.ShapeDtypeStruct((4, 1024, 128), F32),
            jax.ShapeDtypeStruct((16 * 2 * 32, 128), F32),
        ),
        in_specs=[VMEM] * 5,
        out_specs=(VMEM, VMEM),
        scratch_shapes=[
            pltpu.VMEM((4 * SPAN, 128), F32),
            pltpu.VMEM((4 * SPAN, 128), F32),
            pltpu.VMEM((16 * 40, 128), F32),
            pltpu.VMEM((16 * 32, 128), F32),
        ],
        compiler_params=pltpu.CompilerParams(vmem_limit_bytes=14 << 20),
        name="inner",
    )(*operands)


def step_kernel(
    cells, inside, near, rows, deep, r1, r2, r3, r4, w, q, got_in, level, relation, half, refs,
    out, step, fresh, ghosts, pool, edge, weave, got, held, got_sem, held_sem, out_sems,
):
    got_copy = pltpu.make_async_copy(got_in, got, got_sem)
    got_copy.start()
    sources = [
        (r1, T), (r1, 0), (r2, T), (r2, 0), (r3, T), (r3, 0), (r4, T), (r4, 0),
        (w, 8 * T), (q, T), (q, 0), (q, 3 * T), (q, 2 * T), (q, 5 * T), (q, 4 * T), (q, 6 * T),
    ]
    for tile in range(T):
        joined = jnp.concatenate([ref[at + tile] for ref, at in sources], axis=0)
        pool[pl.ds(tile * 128, 128), :] = joined.T

    got_copy.wait()
    low = jnp.min(jnp.min(got[...], axis=0, keepdims=True), axis=1, keepdims=True)
    chosen = COURANT * low
    held[...] = chosen
    step_copy = pltpu.make_async_copy(held, step, held_sem)
    step_copy.start()
    ratio = (0.5 * chosen) / spacing_of(level[...])

    def update(n, carry):
        spot = pl.ds(pl.multiple_of(32 * n, 32), 32)
        for c in range(4):
            fresh[c, spot, :] = cells[c, spot, :] - ratio * inside[c, spot, :]
        return carry

    lax.fori_loop(0, 32, update, 0, unroll=8)
    planes = fresh.reshape(4, 32, 32, 128)
    copies = []

    def send(x, nx, y, ny):
        part = (slice(None), pl.ds(x, nx), pl.ds(y, ny))
        sem = out_sems.at[len(copies)]
        copies.append(pltpu.make_async_copy(planes.at[part], out.at[part], sem))
        copies[-1].start()

    send(2, 28, 8, 16)

    flip = 64 * core_index()
    for face in range(4):
        kind = relation[pl.ds(face, 1), :]
        upper = half[pl.ds(face, 1), :] == 1
        names = [refs[pl.ds(2 * face + m, 1), :] for m in range(2)]
        index = [(name & 127) ^ flip for name in names]
        own = [(kind == 0) | (names[0] < 128)]
        own.append((kind == 0) | (jnp.where(kind == 3, names[1], names[0]) < 128))
        for c in range(4):
            slot = 4 * face + c
            base = ((face ^ 1) * 4 + c) * ROWS
            found = candidates(pool, index, kind, upper, base, edge, weave, slot)
            for g in range(2):
                for m in range(2):
                    at = pl.ds((slot * 2 + g) * 32 + 16 * m, 16)
                    other = found[g][16 * m : 16 * m + 16]
                    ghosts[at, :] = jnp.where(own[m], near[at, :], other)

    def border(face, j):
        def part(c, depth):
            if depth < 0:
                return ghosts[pl.ds(((face * 4 + c) * 2 - depth - 1) * 32 + 8 * j, 8), :]
            if face < 2:
                x = depth if face == 0 else 31 - depth
                return cells[c, pl.ds(32 * x + 8 * j, 8), :]
            if depth < 2:
                return rows[pl.ds((face * 4 + c) * ROWS + 32 * depth + 8 * j, 8), :]
            return deep[pl.ds(((face - 2) * 4 + c) * 64 + 32 * (depth - 2) + 8 * j, 8), :]

        depths = [-2, -1, 0, 1, 2, 3]
        if face % 2 == 1:
            depths = depths[::-1]
        q6 = [[part(c, depth) for c in range(4)] for depth in depths]
        lean = [[0.25 * (q6[i + 1][c] - q6[i - 1][c]) for c in range(4)] for i in range(1, 5)]
        flux = []
        for i in range(1, 4):
            left = [q6[i][c] + lean[i - 1][c] for c in range(4)]
            right = [q6[i + 1][c] - lean[i][c] for c in range(4)]
            flux.append(interface(left, right, 1 + face // 2))
        for i in range(2):
            depth = depths[i + 2]
            where = depth if face % 2 == 0 else 31 - depth
            for c in range(4):
                extra = flux[i + 1][c] - flux[i][c]
                if face < 2:
                    spot = pl.ds(32 * where + 8 * j, 8)
                else:
                    spot = pl.ds(256 * j + where, 8, stride=32)
                fresh[c, spot, :] = fresh[c, spot, :] - ratio * extra

    for face in range(2):
        for j in range(4):
            border(face, j)
    send(0, 2, 8, 16)
    send(30, 2, 8, 16)
    for face in (2, 3):
        for j in range(4):
            border(face, j)
            send(8 * j, 8, 24 * (face - 2), 8)
    step_copy.wait()
    for copy in copies:
        copy.wait()


def advance(*operands):
    return pl.pallas_call(
        step_kernel,
        out_shape=(
            jax.ShapeDtypeStruct((4, 32, 32, 128), F32),
            jax.ShapeDtypeStruct((1, 1), F32),
        ),
        in_specs=[VMEM] * 11 + [ANY] + [VMEM] * 4,
        out_specs=(ANY, ANY),
        scratch_shapes=[
            pltpu.VMEM((4, 1024, 128), F32),
            pltpu.VMEM((16 * 2 * 32, 128), F32),
            pltpu.VMEM((PACK, 128), F32),
            pltpu.VMEM((16 * 40, 128), F32),
            pltpu.VMEM((16 * 32, 128), F32),
            pltpu.VMEM(operands[11].shape, F32),
            pltpu.VMEM((1, 1), F32),
            pltpu.SemaphoreType.DMA(()),
            pltpu.SemaphoreType.DMA(()),
            pltpu.SemaphoreType.DMA((11,)),
        ],
        compiler_params=pltpu.CompilerParams(vmem_limit_bytes=18 << 20),
        name="advance",
    )(*operands)


def two_way(array, chips):
    n = lax.axis_size(AXES)
    pairs = [(i, (i + (2 * chips if i % 2 == 0 else -2 * chips)) % n) for i in range(n)]
    return lax.ppermute(array, AXES, pairs)


def swap_cores(array):
    return lax.ppermute(array, AXES, [(i, i ^ 1) for i in range(lax.axis_size(AXES))])


def cross(array):
    n = lax.axis_size(AXES)
    return lax.ppermute(array, AXES, [(i, (i + (-3 if i % 2 else 3)) % n) for i in range(n)])


def compute(fields, patch_level, relation, face_half, neighbour, send_list):
    level = patch_level.reshape(1, 128)
    flat = fields.reshape(4, 1024, 128)
    kinds, halves = relation.T, face_half.T
    refs = neighbour.transpose(1, 2, 0).reshape(8, 128)
    own, swap, rows, deep = pack(flat, level, send_list[0].T)
    w = swap_cores(swap)

    def blk(array, n, count=1):
        return array[n * T : (n + count) * T]

    def ahead(j):
        return blk(own, j - 2)

    def beside(j):
        return blk(w, j - 1)

    low = jnp.minimum(swap[9 * T :], w[9 * T :])
    r3 = two_way(jnp.concatenate([ahead(6), beside(5), beside(8), low]), 3)
    r2 = two_way(jnp.concatenate([ahead(4), beside(3), ahead(7), beside(6), low]), 2)
    r1 = two_way(jnp.concatenate([ahead(2), beside(1), ahead(5), beside(4), low]), 1)
    low = jnp.minimum(jnp.minimum(low, r1[4 * T :]), jnp.minimum(r2[4 * T :], r3[3 * T :]))
    r4 = two_way(jnp.concatenate([ahead(8), beside(7), low]), 4)
    q = cross(
        jnp.concatenate([ahead(3), beside(2), blk(r1, 2, 2), blk(r2, 2, 2), blk(r3, 2)])
    )
    inside, close = inner(flat, rows, kinds, halves, refs)
    depth = lax.axis_size("patch_2")
    columns = lax.axis_size(("patch_0", "patch_1"))
    low = jnp.minimum(low, r4[2 * T :])
    least = jnp.broadcast_to(low, (2 * columns // 8, 8, 128)).reshape(2 * columns, 128)
    groups = [
        [(r * depth + (g + c) % depth) * 2 + c for r in range(columns) for c in range(2)]
        for g in range(depth)
    ]
    got = lax.all_to_all(least, AXES, 0, 0, tiled=True, axis_index_groups=groups)
    advanced, step = advance(
        flat, inside, close, rows, deep, r1, r2, r3, r4, w, q, got, level, kinds, halves, refs
    )
    return advanced, step[0, 0]


def stepper(mesh):
    split = Mesh(mesh.devices.reshape(SHAPE), AXES)
    return jax.shard_map(
        compute,
        mesh=split,
        in_specs=(
            P(None, None, None, AXES),
            P(AXES),
            P(AXES, None),
            P(AXES, None),
            P(AXES, None, None),
            P(AXES, None, None),
        ),
        out_specs=(P(None, None, None, AXES), P()),
        check_vma=False,
    )


def solution(mesh):
    return stepper(mesh)
```
